32 devices in a mesh: inst: 2 (over x), dev: 4 (over z), side: 4 (over y, core).
Axes of the slice: x: 2, y: 2, z: 4, core: 2. Of those that a mesh axis runs over, the one named last changes fastest.
Arguments:
- hidden: bfloat16 [2048, 4096], P(('inst', 'dev')), parts along dimension 0
- cache_len: int32 [2048], P(('inst', 'dev')), parts along dimension 0
- k_cache: bfloat16 [1, 2048, 8, 64, 128], P(None, ('inst', 'dev')), parts along dimension 1
- v_cache: bfloat16 [1, 2048, 8, 64, 128], P(None, ('inst', 'dev')), parts along dimension 1
- w_q: bfloat16 [1, 4096, 4096], replicated
- w_kv: bfloat16 [1, 4096, 2048], replicated
- w_o: bfloat16 [1, 4096, 4096], replicated
- attn_gain: float32 [1, 4096], replicated
- ffn_gain: float32 [1, 4096], replicated
- w_gate: bfloat16 [1, 4096, 14336], P(None, None, 'dev')
- w_up: bfloat16 [1, 4096, 14336], P(None, None, 'dev')
- w_down: bfloat16 [1, 14336, 4096], P(None, 'dev')
Outputs:
- output: bfloat16 [2048, 4096], P(('inst', 'dev', 'side')), parts along dimension 0
There are 2 independent parts. The reference program is written for one: setup_inputs(seed, part) draws one part's arguments, and reference() takes and returns one part's arrays. A program takes and returns all parts, laid end to end along the dimension named above; an argument that names none is the same for every part.
All inputs are finite; a program needn't handle non-finite values.
Results may differ from the reference program's by a relative error of at most 0.0123253.
Values are sent between devices in bfloat16 or wider.
A program may use at most 1 GiB of HBM per device.

```python
import math
import jax
import jax.numpy as jnp
from jax import lax

D = 4096
FF = 14336
HEADS = 32
KV_HEADS = 8
HEAD = 128
SEQ = 64
LAYERS = 1
BATCH = 1024

EPS = 1e-5
ROPE_BASE = 10000.0
KEY_STD = math.sqrt(1.5 * math.log(SEQ))
GROUP = HEADS // KV_HEADS


def setup_inputs(seed: int = 0, part: int = 0) -> dict:
    base_key = jax.random.key(seed)
    part_key = jax.random.fold_in(base_key, part)
    shared = jax.random.split(base_key, 8)
    local = jax.random.split(part_key, 6)
    hidden = jax.random.normal(local[0], (BATCH, D), jnp.float32)
    cache_len = jax.random.randint(local[1], (BATCH,), 1, SEQ + 1, dtype=jnp.int32)
    cache_len = cache_len.at[0].set(SEQ).at[1].set(1)
    cache_shape = (LAYERS, BATCH, KV_HEADS, SEQ, HEAD)
    mean_shape = (LAYERS, BATCH, KV_HEADS, 1, HEAD)
    pos_ramp = (2.0 * jnp.arange(SEQ, dtype=jnp.float32) / SEQ - 1.0).reshape(1, 1, 1, SEQ, 1)
    k_cache = KEY_STD * jax.random.normal(local[2], cache_shape, jnp.float32)
    v_cache = (jax.random.normal(local[3], cache_shape, jnp.float32)
               + 0.7 * jax.random.normal(local[4], mean_shape, jnp.float32)
               + 0.7 * pos_ramp * jax.random.normal(local[5], mean_shape, jnp.float32))
    kv_cols = KV_HEADS * HEAD
    col_scale = jnp.concatenate([jnp.full((kv_cols,), KEY_STD, jnp.float32), jnp.full((kv_cols,), 2.0, jnp.float32)])
    w_q = jax.random.normal(shared[0], (LAYERS, D, HEADS * HEAD), jnp.float32) * D ** -0.5
    w_kv = jax.random.normal(shared[1], (LAYERS, D, 2 * kv_cols), jnp.float32) * (D ** -0.5) * col_scale
    w_o = jax.random.normal(shared[2], (LAYERS, HEADS * HEAD, D), jnp.float32) * (HEADS * HEAD) ** -0.5
    attn_gain = jax.random.uniform(shared[3], (LAYERS, D), jnp.float32, 0.5, 1.5)
    ffn_gain = jax.random.uniform(shared[4], (LAYERS, D), jnp.float32, 0.5, 1.5)
    w_gate = jax.random.normal(shared[5], (LAYERS, D, FF), jnp.float32) * D ** -0.5
    w_up = jax.random.normal(shared[6], (LAYERS, D, FF), jnp.float32) * D ** -0.5
    w_down = jax.random.normal(shared[7], (LAYERS, FF, D), jnp.float32) * (1.5 * FF ** -0.5)
    return {
        'hidden': hidden.astype(jnp.bfloat16),
        'cache_len': cache_len,
        'k_cache': k_cache.astype(jnp.bfloat16),
        'v_cache': v_cache.astype(jnp.bfloat16),
        'w_q': w_q.astype(jnp.bfloat16),
        'w_kv': w_kv.astype(jnp.bfloat16),
        'w_o': w_o.astype(jnp.bfloat16),
        'attn_gain': attn_gain,
        'ffn_gain': ffn_gain,
        'w_gate': w_gate.astype(jnp.bfloat16),
        'w_up': w_up.astype(jnp.bfloat16),
        'w_down': w_down.astype(jnp.bfloat16),
    }


def rms_norm(rows, gain):
    rows_f = rows.astype(jnp.float32)
    inv_rms = lax.rsqrt(jnp.mean(rows_f * rows_f, axis=-1, keepdims=True) + EPS)
    return (rows_f * inv_rms * gain).astype(jnp.bfloat16)


def rotary(vecs, positions):
    half_dim = vecs.shape[-1] // 2
    freqs = ROPE_BASE ** (-jnp.arange(half_dim, dtype=jnp.float32) / half_dim)
    angle = positions.astype(jnp.float32)[:, None, None] * freqs
    cos_part = jnp.cos(angle)
    sin_part = jnp.sin(angle)
    first = vecs[..., :half_dim]
    second = vecs[..., half_dim:]
    return jnp.concatenate([first * cos_part - second * sin_part, second * cos_part + first * sin_part], axis=-1)


def attend_one(operands):
    q_row, k_new, v_new, k_seq, v_seq, length = operands
    scale = HEAD ** -0.5
    q_f = q_row.astype(jnp.float32)
    scores = jnp.einsum('kgd,ksd->kgs', q_f, k_seq.astype(jnp.float32)) * scale
    valid = jnp.arange(SEQ)[None, None, :] < length
    scores = jnp.where(valid, scores, -1e30)
    self_score = jnp.einsum('kgd,kd->kg', q_f, k_new.astype(jnp.float32)) * scale
    row_max = jnp.maximum(jnp.max(scores, axis=-1), self_score)
    exp_scores = jnp.exp(scores - row_max[..., None])
    self_exp = jnp.exp(self_score - row_max)
    total_exp = jnp.sum(exp_scores, axis=-1) + self_exp
    mixed = jnp.einsum('kgs,ksd->kgd', exp_scores.astype(jnp.bfloat16).astype(jnp.float32), v_seq.astype(jnp.float32))
    mixed = mixed + self_exp.astype(jnp.bfloat16).astype(jnp.float32)[..., None] * v_new.astype(jnp.float32)[:, None, :]
    return (mixed / total_exp[..., None]).astype(jnp.bfloat16)


def reference(hidden, cache_len, k_cache, v_cache, w_q, w_kv, w_o, attn_gain, ffn_gain, w_gate, w_up, w_down):
    def layer_step(x_cur, per_layer):
        q_weight, kv_weight, o_weight, gain_attn, gain_ffn, gate_weight, up_weight, down_weight, k_layer, v_layer = per_layer
        normed = rms_norm(x_cur, gain_attn)
        q_all = jnp.dot(normed, q_weight, preferred_element_type=jnp.float32).reshape(BATCH, HEADS, HEAD)
        kv_all = jnp.dot(normed, kv_weight, preferred_element_type=jnp.float32).reshape(BATCH, 2, KV_HEADS, HEAD)
        q_rows = rotary(q_all, cache_len).astype(jnp.bfloat16).reshape(BATCH, KV_HEADS, GROUP, HEAD)
        k_new = rotary(kv_all[:, 0], cache_len).astype(jnp.bfloat16)
        v_new = kv_all[:, 1].astype(jnp.bfloat16)
        mixed = lax.map(attend_one, (q_rows, k_new, v_new, k_layer, v_layer, cache_len))
        attn_out = jnp.dot(mixed.reshape(BATCH, HEADS * HEAD), o_weight, preferred_element_type=jnp.float32)
        x_mid = (x_cur.astype(jnp.float32) + attn_out).astype(jnp.bfloat16)
        h_rows = rms_norm(x_mid, gain_ffn)
        gate = jnp.dot(h_rows, gate_weight, preferred_element_type=jnp.float32)
        up_proj = jnp.dot(h_rows, up_weight, preferred_element_type=jnp.float32)
        act_rows = (jax.nn.silu(gate) * up_proj).astype(jnp.bfloat16)
        y_rows = jnp.dot(act_rows, down_weight, preferred_element_type=jnp.float32).astype(jnp.bfloat16)
        x_next = (x_mid.astype(jnp.float32) + y_rows.astype(jnp.float32)).astype(jnp.bfloat16)
        return x_next, None

    x_out, _ = lax.scan(layer_step, hidden, (w_q, w_kv, w_o, attn_gain, ffn_gain, w_gate, w_up, w_down, k_cache, v_cache))
    return x_out
```

```python
import jax
import jax.numpy as jnp
from jax import lax
from jax.sharding import PartitionSpec as P

EPS = 1e-5
ROPE_BASE = 10000.0


def rms_norm(rows, gain):
    rows_f = rows.astype(jnp.float32)
    inv_rms = lax.rsqrt(jnp.mean(rows_f * rows_f, axis=-1, keepdims=True) + EPS)
    return (rows_f * inv_rms * gain).astype(jnp.bfloat16)


def rotary(vecs, positions):
    half_dim = vecs.shape[-1] // 2
    freqs = ROPE_BASE ** (-jnp.arange(half_dim, dtype=jnp.float32) / half_dim)
    angle = positions.astype(jnp.float32)[:, None, None] * freqs
    cos_part = jnp.cos(angle)
    sin_part = jnp.sin(angle)
    first = vecs[..., :half_dim]
    second = vecs[..., half_dim:]
    return jnp.concatenate([first * cos_part - second * sin_part, second * cos_part + first * sin_part], axis=-1)


def attention_layer(x_rows, lengths, k_seq, v_seq, q_weight, kv_weight, o_weight, gain_attn):
    count = x_rows.shape[0]
    kv_heads = k_seq.shape[1]
    head_dim = k_seq.shape[-1]
    normed = rms_norm(x_rows, gain_attn)
    q_all = jnp.dot(normed, q_weight, preferred_element_type=jnp.float32).reshape(count, -1, head_dim)
    kv_all = jnp.dot(normed, kv_weight, preferred_element_type=jnp.float32).reshape(count, 2, kv_heads, head_dim)
    q_rows = rotary(q_all, lengths).astype(jnp.bfloat16).reshape(count, kv_heads, -1, head_dim)
    k_new = rotary(kv_all[:, 0], lengths).astype(jnp.bfloat16)
    v_new = kv_all[:, 1].astype(jnp.bfloat16)
    scale = head_dim ** -0.5
    scores = jnp.einsum('nkgd,nksd->nkgs', q_rows, k_seq, preferred_element_type=jnp.float32) * scale
    valid = jnp.arange(k_seq.shape[2])[None, None, None, :] < lengths[:, None, None, None]
    scores = jnp.where(valid, scores, -1e30)
    self_score = jnp.einsum('nkgd,nkd->nkg', q_rows, k_new, preferred_element_type=jnp.float32) * scale
    row_max = jnp.maximum(jnp.max(scores, axis=-1), self_score)
    exp_scores = jnp.exp(scores - row_max[..., None])
    self_exp = jnp.exp(self_score - row_max)
    total_exp = jnp.sum(exp_scores, axis=-1) + self_exp
    mixed = jnp.einsum('nkgs,nksd->nkgd', exp_scores.astype(jnp.bfloat16), v_seq, preferred_element_type=jnp.float32)
    mixed = mixed + self_exp.astype(jnp.bfloat16).astype(jnp.float32)[..., None] * v_new.astype(jnp.float32)[:, :, None, :]
    mixed = (mixed / total_exp[..., None]).astype(jnp.bfloat16).reshape(count, -1)
    attn_out = jnp.dot(mixed, o_weight, preferred_element_type=jnp.float32)
    return (x_rows.astype(jnp.float32) + attn_out).astype(jnp.bfloat16)


def ffn_partial(h_rows, gate_weight, up_weight, down_weight):
    gate = jnp.dot(h_rows, gate_weight, preferred_element_type=jnp.float32)
    up_proj = jnp.dot(h_rows, up_weight, preferred_element_type=jnp.float32)
    act_rows = (jax.nn.silu(gate) * up_proj).astype(jnp.bfloat16)
    return jnp.dot(act_rows, down_weight, preferred_element_type=jnp.float32)


def own_rows(local, side_idx, n_side):
    rows = local.shape[0] // n_side
    return lax.dynamic_slice_in_dim(local, side_idx * rows, rows, axis=0)


def solution(mesh):
    n_side = mesh.shape['side']
    batch_axes = ('inst', 'dev')
    in_specs = (
        P(batch_axes, None),
        P(batch_axes),
        P(None, batch_axes, None, None, None),
        P(None, batch_axes, None, None, None),
        P(), P(), P(), P(), P(),
        P(None, None, 'dev'),
        P(None, None, 'dev'),
        P(None, 'dev', None),
    )
    out_specs = P(('inst', 'dev', 'side'), None)

    def device_fn(hidden, cache_len, k_cache, v_cache, w_q, w_kv, w_o, attn_gain, ffn_gain, w_gate, w_up, w_down):
        side_idx = lax.axis_index('side')
        x_rows = own_rows(hidden, side_idx, n_side)
        lengths = own_rows(cache_len, side_idx, n_side)
        for layer in range(w_q.shape[0]):
            k_seq = own_rows(k_cache[layer], side_idx, n_side)
            v_seq = own_rows(v_cache[layer], side_idx, n_side)
            x_mid = attention_layer(x_rows, lengths, k_seq, v_seq, w_q[layer], w_kv[layer], w_o[layer], attn_gain[layer])
            h_rows = rms_norm(x_mid, ffn_gain[layer])
            h_all = lax.all_gather(h_rows, 'dev', axis=0, tiled=True)
            part_sum = ffn_partial(h_all, w_gate[layer], w_up[layer], w_down[layer])
            summed = lax.psum_scatter(part_sum, 'dev', scatter_dimension=0, tiled=True)
            x_rows = (x_mid.astype(jnp.float32) + summed.astype(jnp.bfloat16).astype(jnp.float32)).astype(jnp.bfloat16)
        return x_rows

    return jax.shard_map(device_fn, mesh=mesh, in_specs=in_specs, out_specs=out_specs, check_vma=False)
```

```python
import functools

import jax
import jax.numpy as jnp
from jax import lax
from jax.experimental import pallas as pl
from jax.experimental.pallas import tpu as pltpu
from jax.sharding import PartitionSpec as P

EPS = 1e-5
ROPE_BASE = 10000.0
TILE = 512
SLOTS = 10
SEQS = 8
KV_BUFS = 3
VMEM_LIMIT = 66_000_000


def attention_kernel(rows, x_ref, gain_ref, ffn_gain_ref, cos_ref, sin_ref, len_ref, k_hbm, v_hbm, wq_hbm, wkv_hbm,
                     wo_hbm, x1_ref, h_ref, ring, k_buf, v_buf, a_s, q_s, kv_s, o_s, ob_s, tq, tk, tv, to,
                     w_sem, k_sem, v_sem):
    width = x_ref.shape[1]
    kv_heads, cache, head = k_hbm.shape[1:]
    n_q = wq_hbm.shape[1] // TILE
    n_kv = wkv_hbm.shape[1] // TILE
    n_o = wo_hbm.shape[1] // TILE
    heads = wq_hbm.shape[1] // head
    group = heads // kv_heads
    n_groups = rows // SEQS
    base = lax.axis_index('side') * rows

    def weight_copy(hbm, tile, slot):
        cols = pl.ds(pl.multiple_of(tile * TILE, TILE), TILE)
        return pltpu.make_async_copy(hbm.at[:, cols], ring.at[slot], w_sem.at[slot])

    def kv_copies(g):
        buf = lax.rem(g, KV_BUFS)
        seqs = pl.ds(base + g * SEQS, SEQS)
        return (pltpu.make_async_copy(k_hbm.at[seqs], k_buf.at[buf], k_sem.at[buf]),
                pltpu.make_async_copy(v_hbm.at[seqs], v_buf.at[buf], v_sem.at[buf]))

    def start_kv(g):
        for copy in kv_copies(g):
            copy.start()

    def start_seq(i):
        slot = lax.rem(i, SLOTS)

        @pl.when(i < n_q)
        def _():
            weight_copy(wq_hbm, i, slot).start()

        @pl.when((i >= n_q) & (i < n_q + n_kv))
        def _():
            weight_copy(wkv_hbm, i - n_q, slot).start()

        @pl.when((i >= n_q + n_kv) & (i < n_q + n_kv + n_o))
        def _():
            weight_copy(wo_hbm, i - n_q - n_kv, slot).start()

    def first(i, carry):
        start_seq(i)
        return carry

    lax.fori_loop(0, SLOTS, first, 0)
    for g in range(KV_BUFS):
        start_kv(g)

    x_f = x_ref[...].astype(jnp.float32)
    inv = lax.rsqrt(jnp.mean(x_f * x_f, axis=-1, keepdims=True) + EPS)
    a_s[...] = (x_f * inv * gain_ref[...]).astype(jnp.bfloat16)

    def rotated(tile, i):
        vec = tile[:, i * head:(i + 1) * head]
        return vec * cos_ref[...] + pltpu.roll(vec, head // 2, 1) * sin_ref[...]

    def q_step(t, carry):
        slot = lax.rem(t, SLOTS)
        weight_copy(wq_hbm, t, slot).wait()
        tile = jnp.dot(a_s[...], ring[slot], preferred_element_type=jnp.float32)
        for i in range(TILE // head):
            q_s[:, pl.ds(pl.multiple_of(t * TILE + i * head, head), head)] = rotated(tile, i)
        start_seq(t + SLOTS)
        return carry

    lax.fori_loop(0, n_q, q_step, 0)

    def kv_step(t, carry):
        slot = lax.rem(t + n_q, SLOTS)
        weight_copy(wkv_hbm, t, slot).wait()
        tile = jnp.dot(a_s[...], ring[slot], preferred_element_type=jnp.float32)

        @pl.when(t < n_kv // 2)
        def _():
            for i in range(TILE // head):
                kv_s[:, pl.ds(pl.multiple_of(t * TILE + i * head, head), head)] = rotated(tile, i)

        @pl.when(t >= n_kv // 2)
        def _():
            kv_s[:, pl.ds(pl.multiple_of(t * TILE, TILE), TILE)] = tile

        start_seq(t + n_q + SLOTS)
        return carry

    lax.fori_loop(0, n_kv, kv_step, 0)

    scale = head ** -0.5
    keys = kv_heads * cache
    row_head = lax.broadcasted_iota(jnp.int32, (heads, keys), 0) // group
    col = lax.broadcasted_iota(jnp.int32, (heads, keys), 1)
    key_pos = jnp.where(col // cache == row_head, col % cache, cache + 1)
    own = (lax.broadcasted_iota(jnp.int32, (heads, kv_heads), 0) // group
           == lax.broadcasted_iota(jnp.int32, (heads, kv_heads), 1))
    nt = (((1,), (1,)), ((), ()))

    def kv_group(g, carry):
        buf = lax.rem(g, KV_BUFS)
        block = pl.ds(pl.multiple_of(g * SEQS, SEQS), SEQS)
        for h in range(heads):
            tq[pl.ds(h, SEQS, stride=heads), :] = q_s[block, h * head:(h + 1) * head]
        for h in range(kv_heads):
            tk[pl.ds(h, SEQS, stride=kv_heads), :] = kv_s[block, h * head:(h + 1) * head]
            off = (kv_heads + h) * head
            tv[pl.ds(h, SEQS, stride=kv_heads), :] = kv_s[block, off:off + head]
        for copy in kv_copies(g):
            copy.wait()
        for i in range(SEQS):
            n = len_ref[g * SEQS + i]
            q = tq[i * heads:(i + 1) * heads, :].astype(jnp.bfloat16)
            k_new = tk[i * kv_heads:(i + 1) * kv_heads, :].astype(jnp.bfloat16)
            v_new = tv[i * kv_heads:(i + 1) * kv_heads, :].astype(jnp.bfloat16)
            k = k_buf[buf, i].reshape(keys, head)
            v = v_buf[buf, i].reshape(keys, head)
            s = lax.dot_general(q, k, nt, preferred_element_type=jnp.float32) * scale
            s = jnp.where(key_pos < n, s, -1e30)
            s_own = lax.dot_general(q, k_new, nt, preferred_element_type=jnp.float32) * scale
            s_own = jnp.max(jnp.where(own, s_own, -jnp.inf), axis=-1, keepdims=True)
            top = jnp.maximum(jnp.max(s, axis=-1, keepdims=True), s_own)
            e = jnp.exp(s - top)
            e_own = jnp.exp(s_own - top)
            total = jnp.sum(e, axis=-1, keepdims=True) + e_own
            mixed = jnp.dot(e.astype(jnp.bfloat16), v, preferred_element_type=jnp.float32)
            spread = jnp.where(own, e_own, 0.0).astype(jnp.bfloat16)
            mixed += jnp.dot(spread, v_new, preferred_element_type=jnp.float32)
            to[i * heads:(i + 1) * heads, :] = mixed / total
        for h in range(heads):
            o_s[block, h * head:(h + 1) * head] = to[pl.ds(h, SEQS, stride=heads), :]

        @pl.when(g + KV_BUFS < n_groups)
        def _():
            start_kv(g + KV_BUFS)

        return carry

    lax.fori_loop(0, n_groups, kv_group, 0)
    ob_s[...] = o_s[...].astype(jnp.bfloat16)

    def o_step(t, square):
        slot = lax.rem(t + n_q + n_kv, SLOTS)
        weight_copy(wo_hbm, t, slot).wait()
        tile = jnp.dot(ob_s[...], ring[slot], preferred_element_type=jnp.float32)
        cols = pl.ds(pl.multiple_of(t * TILE, TILE), TILE)
        x1 = (x_ref[:, cols].astype(jnp.float32) + tile).astype(jnp.bfloat16)
        x1_ref[:, cols] = x1
        x1_f = x1.astype(jnp.float32)
        return square + jnp.sum(x1_f * x1_f, axis=-1, keepdims=True)

    square = lax.fori_loop(0, n_o, o_step, jnp.zeros((rows, 1), jnp.float32))
    inv = lax.rsqrt(square / width + EPS)
    h_ref[...] = (x1_ref[...].astype(jnp.float32) * inv * ffn_gain_ref[...]).astype(jnp.bfloat16)


def attention(x_rows, lengths, k_cache, v_cache, w_q, w_kv, w_o, gain_attn, gain_ffn):
    rows, width = x_rows.shape
    _, kv_heads, cache, head = k_cache.shape
    heads = w_q.shape[1] // head
    half = head // 2
    freqs = ROPE_BASE ** (-jnp.arange(half, dtype=jnp.float32) / half)
    angle = lengths.astype(jnp.float32)[:, None] * freqs
    cos_part, sin_part = jnp.cos(angle), jnp.sin(angle)
    cos_full = jnp.concatenate([cos_part, cos_part], axis=-1)
    sin_full = jnp.concatenate([-sin_part, sin_part], axis=-1)
    vmem = pl.BlockSpec(memory_space=pltpu.VMEM)
    hbm = pl.BlockSpec(memory_space=pl.ANY)
    row_block = jax.ShapeDtypeStruct((rows, width), jnp.bfloat16)
    weights = w_q.size + w_kv.size + w_o.size
    return pl.pallas_call(
        functools.partial(attention_kernel, rows),
        out_shape=(row_block, row_block),
        in_specs=[vmem] * 5 + [pl.BlockSpec(memory_space=pltpu.SMEM)] + [hbm] * 5,
        out_specs=(vmem, vmem),
        scratch_shapes=[
            pltpu.VMEM((SLOTS, width, TILE), jnp.bfloat16),
            pltpu.VMEM((KV_BUFS, SEQS, kv_heads, cache, head), jnp.bfloat16),
            pltpu.VMEM((KV_BUFS, SEQS, kv_heads, cache, head), jnp.bfloat16),
            pltpu.VMEM((rows, width), jnp.bfloat16),
            pltpu.VMEM((rows, heads * head), jnp.float32),
            pltpu.VMEM((rows, 2 * kv_heads * head), jnp.float32),
            pltpu.VMEM((rows, heads * head), jnp.float32),
            pltpu.VMEM((rows, heads * head), jnp.bfloat16),
            pltpu.VMEM((SEQS * heads, head), jnp.float32),
            pltpu.VMEM((SEQS * kv_heads, head), jnp.float32),
            pltpu.VMEM((SEQS * kv_heads, head), jnp.float32),
            pltpu.VMEM((SEQS * heads, head), jnp.float32),
            pltpu.SemaphoreType.DMA((SLOTS,)),
            pltpu.SemaphoreType.DMA((KV_BUFS,)),
            pltpu.SemaphoreType.DMA((KV_BUFS,)),
        ],
        compiler_params=pltpu.CompilerParams(vmem_limit_bytes=VMEM_LIMIT),
        cost_estimate=pl.CostEstimate(flops=2 * rows * weights, bytes_accessed=2 * weights, transcendentals=0),
        name="attention",
    )(x_rows, gain_attn[None], gain_ffn[None], cos_full, sin_full, lengths, k_cache, v_cache, w_q, w_kv, w_o)


def ffn_partial(h_rows, gate_weight, up_weight, down_weight):
    gate = jnp.dot(h_rows, gate_weight, preferred_element_type=jnp.float32)
    up_proj = jnp.dot(h_rows, up_weight, preferred_element_type=jnp.float32)
    act_rows = (jax.nn.silu(gate) * up_proj).astype(jnp.bfloat16)
    return jnp.dot(act_rows, down_weight, preferred_element_type=jnp.float32)


def own_rows(local, side_idx, n_side):
    rows = local.shape[0] // n_side
    return lax.dynamic_slice_in_dim(local, side_idx * rows, rows, axis=0)


def solution(mesh):
    n_side = mesh.shape['side']
    batch_axes = ('inst', 'dev')
    in_specs = (
        P(batch_axes, None),
        P(batch_axes),
        P(None, batch_axes, None, None, None),
        P(None, batch_axes, None, None, None),
        P(), P(), P(), P(), P(),
        P(None, None, 'dev'),
        P(None, None, 'dev'),
        P(None, 'dev', None),
    )
    out_specs = P(('inst', 'dev', 'side'), None)

    def device_fn(hidden, cache_len, k_cache, v_cache, w_q, w_kv, w_o, attn_gain, ffn_gain, w_gate, w_up, w_down):
        side_idx = lax.axis_index('side')
        x_rows = own_rows(hidden, side_idx, n_side)
        lengths = own_rows(cache_len, side_idx, n_side)
        for layer in range(w_q.shape[0]):
            x_mid, h_rows = attention(x_rows, lengths, k_cache[layer], v_cache[layer], w_q[layer], w_kv[layer], w_o[layer],
                                      attn_gain[layer], ffn_gain[layer])
            h_all = lax.all_gather(h_rows, 'dev', axis=0, tiled=True)
            part_sum = ffn_partial(h_all, w_gate[layer], w_up[layer], w_down[layer])
            summed = lax.psum_scatter(part_sum, 'dev', scatter_dimension=0, tiled=True)
            x_rows = (x_mid.astype(jnp.float32) + summed.astype(jnp.bfloat16).astype(jnp.float32)).astype(jnp.bfloat16)
        return x_rows

    return jax.shard_map(device_fn, mesh=mesh, in_specs=in_specs, out_specs=out_specs, check_vma=False)
```

```python
import functools

import jax
import jax.numpy as jnp
from jax import lax
from jax.experimental import pallas as pl
from jax.experimental.pallas import tpu as pltpu
from jax.sharding import PartitionSpec as P

EPS = 1e-5
ROPE_BASE = 10000.0
TILE = 512
SLOTS = 10
SEQS = 8
KV_BUFS = 3
VMEM_LIMIT = 66_000_000


def attention_kernel(rows, x_ref, gain_ref, ffn_gain_ref, cos_ref, sin_ref, len_ref, k_hbm, v_hbm, wq_hbm, wkv_hbm,
                     wo_hbm, x1_ref, h_ref, ring, k_buf, v_buf, a_s, q_s, kv_s, o_s, ob_s, tq, tk, tv, to,
                     w_sem, k_sem, v_sem):
    width = x_ref.shape[1]
    kv_heads, cache, head = k_hbm.shape[1:]
    n_q = wq_hbm.shape[1] // TILE
    n_kv = wkv_hbm.shape[1] // TILE
    n_o = wo_hbm.shape[1] // TILE
    heads = wq_hbm.shape[1] // head
    group = heads // kv_heads
    n_groups = rows // SEQS
    base = lax.axis_index('side') * rows

    def weight_copy(hbm, tile, slot):
        cols = pl.ds(pl.multiple_of(tile * TILE, TILE), TILE)
        return pltpu.make_async_copy(hbm.at[:, cols], ring.at[slot], w_sem.at[slot])

    def kv_copies(g):
        buf = lax.rem(g, KV_BUFS)
        seqs = pl.ds(base + g * SEQS, SEQS)
        return (pltpu.make_async_copy(k_hbm.at[seqs], k_buf.at[buf], k_sem.at[buf]),
                pltpu.make_async_copy(v_hbm.at[seqs], v_buf.at[buf], v_sem.at[buf]))

    def start_kv(g):
        for copy in kv_copies(g):
            copy.start()

    def start_seq(i):
        slot = lax.rem(i, SLOTS)

        @pl.when(i < n_q)
        def _():
            weight_copy(wq_hbm, i, slot).start()

        @pl.when((i >= n_q) & (i < n_q + n_kv))
        def _():
            weight_copy(wkv_hbm, i - n_q, slot).start()

        @pl.when((i >= n_q + n_kv) & (i < n_q + n_kv + n_o))
        def _():
            weight_copy(wo_hbm, i - n_q - n_kv, slot).start()

    def first(i, carry):
        start_seq(i)
        return carry

    lax.fori_loop(0, SLOTS, first, 0)
    for g in range(KV_BUFS):
        start_kv(g)

    x_f = x_ref[...].astype(jnp.float32)
    inv = lax.rsqrt(jnp.mean(x_f * x_f, axis=-1, keepdims=True) + EPS)
    a_s[...] = (x_f * inv * gain_ref[...]).astype(jnp.bfloat16)

    def rotated(tile, i):
        vec = tile[:, i * head:(i + 1) * head]
        return vec * cos_ref[...] + pltpu.roll(vec, head // 2, 1) * sin_ref[...]

    def q_step(t, carry):
        slot = lax.rem(t, SLOTS)
        weight_copy(wq_hbm, t, slot).wait()
        tile = jnp.dot(a_s[...], ring[slot], preferred_element_type=jnp.float32)
        for i in range(TILE // head):
            q_s[:, pl.ds(pl.multiple_of(t * TILE + i * head, head), head)] = rotated(tile, i)
        start_seq(t + SLOTS)
        return carry

    lax.fori_loop(0, n_q, q_step, 0)

    def kv_step(t, carry):
        slot = lax.rem(t + n_q, SLOTS)
        weight_copy(wkv_hbm, t, slot).wait()
        tile = jnp.dot(a_s[...], ring[slot], preferred_element_type=jnp.float32)

        @pl.when(t < n_kv // 2)
        def _():
            for i in range(TILE // head):
                kv_s[:, pl.ds(pl.multiple_of(t * TILE + i * head, head), head)] = rotated(tile, i)

        @pl.when(t >= n_kv // 2)
        def _():
            kv_s[:, pl.ds(pl.multiple_of(t * TILE, TILE), TILE)] = tile

        start_seq(t + n_q + SLOTS)
        return carry

    lax.fori_loop(0, n_kv, kv_step, 0)

    scale = head ** -0.5
    keys = kv_heads * cache
    row_head = lax.broadcasted_iota(jnp.int32, (heads, keys), 0) // group
    col = lax.broadcasted_iota(jnp.int32, (heads, keys), 1)
    key_pos = jnp.where(col // cache == row_head, col % cache, cache + 1)
    own = (lax.broadcasted_iota(jnp.int32, (heads, kv_heads), 0) // group
           == lax.broadcasted_iota(jnp.int32, (heads, kv_heads), 1))
    nt = (((1,), (1,)), ((), ()))

    def kv_group(g, carry):
        buf = lax.rem(g, KV_BUFS)
        block = pl.ds(pl.multiple_of(g * SEQS, SEQS), SEQS)
        for h in range(heads):
            tq[pl.ds(h, SEQS, stride=heads), :] = q_s[block, h * head:(h + 1) * head]
        for h in range(kv_heads):
            tk[pl.ds(h, SEQS, stride=kv_heads), :] = kv_s[block, h * head:(h + 1) * head]
            off = (kv_heads + h) * head
            tv[pl.ds(h, SEQS, stride=kv_heads), :] = kv_s[block, off:off + head]
        for copy in kv_copies(g):
            copy.wait()
        for i in range(SEQS):
            n = len_ref[g * SEQS + i]
            q = tq[i * heads:(i + 1) * heads, :].astype(jnp.bfloat16)
            k_new = tk[i * kv_heads:(i + 1) * kv_heads, :].astype(jnp.bfloat16)
            v_new = tv[i * kv_heads:(i + 1) * kv_heads, :].astype(jnp.bfloat16)
            k = k_buf[buf, i].reshape(keys, head)
            v = v_buf[buf, i].reshape(keys, head)
            s = lax.dot_general(q, k, nt, preferred_element_type=jnp.float32) * scale
            s = jnp.where(key_pos < n, s, -1e30)
            s_own = lax.dot_general(q, k_new, nt, preferred_element_type=jnp.float32) * scale
            s_own = jnp.max(jnp.where(own, s_own, -jnp.inf), axis=-1, keepdims=True)
            top = jnp.maximum(jnp.max(s, axis=-1, keepdims=True), s_own)
            e = jnp.exp(s - top)
            e_own = jnp.exp(s_own - top)
            total = jnp.sum(e, axis=-1, keepdims=True) + e_own
            mixed = jnp.dot(e.astype(jnp.bfloat16), v, preferred_element_type=jnp.float32)
            spread = jnp.where(own, e_own, 0.0).astype(jnp.bfloat16)
            mixed += jnp.dot(spread, v_new, preferred_element_type=jnp.float32)
            to[i * heads:(i + 1) * heads, :] = mixed / total
        for h in range(heads):
            o_s[block, h * head:(h + 1) * head] = to[pl.ds(h, SEQS, stride=heads), :]

        @pl.when(g + KV_BUFS < n_groups)
        def _():
            start_kv(g + KV_BUFS)

        return carry

    lax.fori_loop(0, n_groups, kv_group, 0)
    ob_s[...] = o_s[...].astype(jnp.bfloat16)

    def o_step(t, square):
        slot = lax.rem(t + n_q + n_kv, SLOTS)
        weight_copy(wo_hbm, t, slot).wait()
        tile = jnp.dot(ob_s[...], ring[slot], preferred_element_type=jnp.float32)
        cols = pl.ds(pl.multiple_of(t * TILE, TILE), TILE)
        x1 = (x_ref[:, cols].astype(jnp.float32) + tile).astype(jnp.bfloat16)
        x1_ref[:, cols] = x1
        x1_f = x1.astype(jnp.float32)
        return square + jnp.sum(x1_f * x1_f, axis=-1, keepdims=True)

    square = lax.fori_loop(0, n_o, o_step, jnp.zeros((rows, 1), jnp.float32))
    inv = lax.rsqrt(square / width + EPS)
    h_ref[...] = (x1_ref[...].astype(jnp.float32) * inv * ffn_gain_ref[...]).astype(jnp.bfloat16)


def attention(x_rows, lengths, k_cache, v_cache, w_q, w_kv, w_o, gain_attn, gain_ffn):
    rows, width = x_rows.shape
    _, kv_heads, cache, head = k_cache.shape
    heads = w_q.shape[1] // head
    half = head // 2
    freqs = ROPE_BASE ** (-jnp.arange(half, dtype=jnp.float32) / half)
    angle = lengths.astype(jnp.float32)[:, None] * freqs
    cos_part, sin_part = jnp.cos(angle), jnp.sin(angle)
    cos_full = jnp.concatenate([cos_part, cos_part], axis=-1)
    sin_full = jnp.concatenate([-sin_part, sin_part], axis=-1)
    vmem = pl.BlockSpec(memory_space=pltpu.VMEM)
    hbm = pl.BlockSpec(memory_space=pl.ANY)
    row_block = jax.ShapeDtypeStruct((rows, width), jnp.bfloat16)
    weights = w_q.size + w_kv.size + w_o.size
    return pl.pallas_call(
        functools.partial(attention_kernel, rows),
        out_shape=(row_block, row_block),
        in_specs=[vmem] * 5 + [pl.BlockSpec(memory_space=pltpu.SMEM)] + [hbm] * 5,
        out_specs=(vmem, vmem),
        scratch_shapes=[
            pltpu.VMEM((SLOTS, width, TILE), jnp.bfloat16),
            pltpu.VMEM((KV_BUFS, SEQS, kv_heads, cache, head), jnp.bfloat16),
            pltpu.VMEM((KV_BUFS, SEQS, kv_heads, cache, head), jnp.bfloat16),
            pltpu.VMEM((rows, width), jnp.bfloat16),
            pltpu.VMEM((rows, heads * head), jnp.float32),
            pltpu.VMEM((rows, 2 * kv_heads * head), jnp.float32),
            pltpu.VMEM((rows, heads * head), jnp.float32),
            pltpu.VMEM((rows, heads * head), jnp.bfloat16),
            pltpu.VMEM((SEQS * heads, head), jnp.float32),
            pltpu.VMEM((SEQS * kv_heads, head), jnp.float32),
            pltpu.VMEM((SEQS * kv_heads, head), jnp.float32),
            pltpu.VMEM((SEQS * heads, head), jnp.float32),
            pltpu.SemaphoreType.DMA((SLOTS,)),
            pltpu.SemaphoreType.DMA((KV_BUFS,)),
            pltpu.SemaphoreType.DMA((KV_BUFS,)),
        ],
        compiler_params=pltpu.CompilerParams(vmem_limit_bytes=VMEM_LIMIT),
        cost_estimate=pl.CostEstimate(flops=2 * rows * weights, bytes_accessed=2 * weights, transcendentals=0),
        name="attention",
    )(x_rows, gain_attn[None], gain_ffn[None], cos_full, sin_full, lengths, k_cache, v_cache, w_q, w_kv, w_o)


FFN_SLOTS = 10


def ffn_kernel(h_ref, x1_ref, wg_hbm, wu_hbm, wd_hbm, out_ref, ring, h_all, u_s, part, recv,
               w_sem, h_send, h_recv, p_send, p_recv):
    rows, width = h_ref.shape
    depth = wd_hbm.shape[0]
    n_ff = depth // TILE
    n_col = width // TILE
    per_pass = 2 * n_ff + n_col
    dev = lax.axis_index('dev')
    flip = dev >= 2
    is_end = (dev == 0) | (dev == 3)
    is_mid = (dev == 1) | (dev == 2)
    me = jnp.where(is_end, 0, 1)
    end_dev = jnp.where(flip, 3, 0)
    mid_dev = jnp.where(flip, 2, 1)
    far_dev = jnp.where(flip, 1, 2)

    def gate_copy(t, slot):
        cols = pl.ds(pl.multiple_of(t * TILE, TILE), TILE)
        return pltpu.make_async_copy(wg_hbm.at[:, cols], ring.at[slot], w_sem.at[slot])

    def up_copy(t, slot):
        cols = pl.ds(pl.multiple_of(t * TILE, TILE), TILE)
        return pltpu.make_async_copy(wu_hbm.at[:, cols], ring.at[slot], w_sem.at[slot])

    def down_copy(t, slot):
        cols = pl.ds(pl.multiple_of(t * TILE, TILE), TILE)
        return pltpu.make_async_copy(wd_hbm.at[:, cols], ring.at[slot, pl.ds(0, depth)], w_sem.at[slot])

    def start_tile(i):
        slot = lax.rem(i, FFN_SLOTS)
        r = lax.rem(i, per_pass)
        live = i < 2 * per_pass

        @pl.when(live & (r < 2 * n_ff) & (lax.rem(r, 2) == 0))
        def _():
            gate_copy(r // 2, slot).start()

        @pl.when(live & (r < 2 * n_ff) & (lax.rem(r, 2) == 1))
        def _():
            up_copy(r // 2, slot).start()

        @pl.when(live & (r >= 2 * n_ff))
        def _():
            down_copy(r - 2 * n_ff, slot).start()

    def first(i, carry):
        start_tile(i)
        return carry

    lax.fori_loop(0, FFN_SLOTS, first, 0)

    def send_h(src, block, k, target):
        return pltpu.make_async_remote_copy(
            src_ref=src, dst_ref=h_all.at[block], send_sem=h_send.at[k], recv_sem=h_recv.at[block],
            device_id={'dev': target}, device_id_type=pl.DeviceIdType.MESH)

    def send_part(j, c, slot, target):
        return pltpu.make_async_remote_copy(
            src_ref=part.at[j, c], dst_ref=recv.at[slot, c], send_sem=p_send.at[j, c], recv_sem=p_recv.at[slot, c],
            device_id={'dev': target}, device_id_type=pl.DeviceIdType.MESH)

    def signal(target):
        pl.semaphore_signal(pltpu.get_barrier_semaphore(), inc=1, device_id={'dev': target},
                            device_id_type=pl.DeviceIdType.MESH)

    @pl.when(is_end)
    def _():
        signal(mid_dev)
        pl.semaphore_wait(pltpu.get_barrier_semaphore(), 1)
        send_h(h_ref, 0, 0, mid_dev).start()

    @pl.when(is_mid)
    def _():
        signal(end_dev)
        signal(far_dev)
        pl.semaphore_wait(pltpu.get_barrier_semaphore(), 2)
        send_h(h_ref, 1, 0, end_dev).start()
        send_h(h_ref, 2, 1, far_dev).start()

    h_all[me] = h_ref[...]

    @pl.when(is_end)
    def _():
        send_h(h_ref, 1, 0, mid_dev).wait_recv()

    @pl.when(is_mid)
    def _():
        send_h(h_ref, 0, 0, end_dev).wait_recv()
        send_h(h_all.at[0], 3, 2, far_dev).start()
        send_h(h_ref, 2, 0, end_dev).wait_recv()
        send_h(h_all.at[2], 2, 3, end_dev).start()

    for half in range(2):
        def ff_step(t, carry):
            i = half * per_pass + 2 * t
            slot_g, slot_u = lax.rem(i, FFN_SLOTS), lax.rem(i + 1, FFN_SLOTS)
            h = h_all[2 * half:2 * half + 2].reshape(2 * rows, width)
            gate_copy(t, slot_g).wait()
            gate = jnp.dot(h, ring[slot_g], preferred_element_type=jnp.float32)
            start_tile(i + FFN_SLOTS)
            up_copy(t, slot_u).wait()
            up = jnp.dot(h, ring[slot_u], preferred_element_type=jnp.float32)
            start_tile(i + 1 + FFN_SLOTS)
            u_s[:, pl.ds(pl.multiple_of(t * TILE, TILE), TILE)] = (jax.nn.silu(gate) * up).astype(jnp.bfloat16)
            return carry

        def down_step(c, carry):
            i = half * per_pass + 2 * n_ff + c
            slot = lax.rem(i, FFN_SLOTS)
            down_copy(c, slot).wait()
            y = jnp.dot(u_s[...], ring[slot, :depth], preferred_element_type=jnp.float32)
            start_tile(i + FFN_SLOTS)
            part[2 * half, c] = y[:rows]
            part[2 * half + 1, c] = y[rows:]

            @pl.when(is_end)
            def _():
                send_part(2 * half + 1, c, 2 * half, mid_dev).start()

            if half == 0:
                @pl.when(is_mid & (c == n_col - 3))
                def _():
                    send_h(h_ref, 3, 0, end_dev).wait_recv()
                    send_h(h_all.at[3], 3, 4, end_dev).start()

            return carry

        if half == 1:
            @pl.when(is_end)
            def _():
                send_h(h_ref, 2, 0, mid_dev).wait_recv()
                send_h(h_ref, 3, 0, mid_dev).wait_recv()

        lax.fori_loop(0, n_ff, ff_step, 0)
        lax.fori_loop(0, n_col, down_step, 0)

    def finish(c, y):
        cols = pl.ds(pl.multiple_of(c * TILE, TILE), TILE)
        y = y.astype(jnp.bfloat16).astype(jnp.float32)
        out_ref[:, cols] = (x1_ref[:, cols].astype(jnp.float32) + y).astype(jnp.bfloat16)

    @pl.when(is_end)
    def _():
        def second(c, carry):
            send_part(2, c, 1, mid_dev).start()
            return carry

        def home(c, carry):
            send_part(0, c, 0, mid_dev).wait_recv()
            finish(c, part[0, c] + recv[0, c])
            return carry

        def drain(c, carry):
            for j in (1, 3, 2):
                send_part(j, c, 0, mid_dev).wait_send()
            return carry

        lax.fori_loop(0, n_col, second, 0)
        lax.fori_loop(0, n_col, home, 0)
        lax.fori_loop(0, n_col, drain, 0)
        send_h(h_ref, 0, 0, mid_dev).wait_send()

    @pl.when(is_mid)
    def _():
        def back(c):
            send_part(0, c, 4, far_dev).wait_recv()
            part[0, c] += recv[4, c]
            send_part(0, c, 0, end_dev).start()

        def across(c, carry):
            send_part(3, c, 2, end_dev).wait_recv()
            part[3, c] += recv[2, c]
            send_part(3, c, 4, far_dev).start()

            @pl.when(c > 0)
            def _():
                back(c - 1)

            return carry

        def home(c):
            send_part(1, c, 0, end_dev).wait_recv()
            send_part(1, c, 3, far_dev).wait_recv()
            finish(c, part[1, c] + recv[0, c] + recv[3, c])

        def near(c, carry):
            send_part(2, c, 1, end_dev).wait_recv()
            part[2, c] += recv[1, c]
            send_part(2, c, 3, far_dev).start()

            @pl.when(c > 0)
            def _():
                home(c - 1)

            return carry

        def drain(c, carry):
            for j in (3, 0, 2):
                send_part(j, c, 0, far_dev).wait_send()
            return carry

        lax.fori_loop(0, n_col, across, 0)
        back(n_col - 1)
        lax.fori_loop(0, n_col, near, 0)
        home(n_col - 1)
        lax.fori_loop(0, n_col, drain, 0)
        for k in range(5):
            send_h(h_ref, 0, k, end_dev).wait_send()


def ffn(h_rows, x_mid, w_gate, w_up, w_down):
    rows, width = h_rows.shape
    depth = w_down.shape[0]
    n_col = width // TILE
    vmem = pl.BlockSpec(memory_space=pltpu.VMEM)
    hbm = pl.BlockSpec(memory_space=pl.ANY)
    weights = 3 * w_gate.size
    return pl.pallas_call(
        ffn_kernel,
        out_shape=jax.ShapeDtypeStruct((rows, width), jnp.bfloat16),
        in_specs=[vmem, vmem, hbm, hbm, hbm],
        out_specs=vmem,
        scratch_shapes=[
            pltpu.VMEM((FFN_SLOTS, width, TILE), jnp.bfloat16),
            pltpu.VMEM((4, rows, width), jnp.bfloat16),
            pltpu.VMEM((2 * rows, depth), jnp.bfloat16),
            pltpu.VMEM((4, n_col, rows, TILE), jnp.float32),
            pltpu.VMEM((5, n_col, rows, TILE), jnp.float32),
            pltpu.SemaphoreType.DMA((FFN_SLOTS,)),
            pltpu.SemaphoreType.DMA((5,)),
            pltpu.SemaphoreType.DMA((4,)),
            pltpu.SemaphoreType.DMA((4, n_col)),
            pltpu.SemaphoreType.DMA((5, n_col)),
        ],
        compiler_params=pltpu.CompilerParams(vmem_limit_bytes=VMEM_LIMIT, collective_id=0, has_side_effects=True),
        cost_estimate=pl.CostEstimate(flops=8 * rows * weights, bytes_accessed=4 * weights, transcendentals=0),
        name="ffn",
    )(h_rows, x_mid, w_gate, w_up, w_down)


def own_rows(local, side_idx, n_side):
    rows = local.shape[0] // n_side
    return lax.dynamic_slice_in_dim(local, side_idx * rows, rows, axis=0)


def solution(mesh):
    n_side = mesh.shape['side']
    batch_axes = ('inst', 'dev')
    in_specs = (
        P(batch_axes, None),
        P(batch_axes),
        P(None, batch_axes, None, None, None),
        P(None, batch_axes, None, None, None),
        P(), P(), P(), P(), P(),
        P(None, None, 'dev'),
        P(None, None, 'dev'),
        P(None, 'dev', None),
    )
    out_specs = P(('inst', 'dev', 'side'), None)

    def device_fn(hidden, cache_len, k_cache, v_cache, w_q, w_kv, w_o, attn_gain, ffn_gain, w_gate, w_up, w_down):
        side_idx = lax.axis_index('side')
        x_rows = own_rows(hidden, side_idx, n_side)
        lengths = own_rows(cache_len, side_idx, n_side)
        for layer in range(w_q.shape[0]):
            x_mid, h_rows = attention(x_rows, lengths, k_cache[layer], v_cache[layer], w_q[layer], w_kv[layer], w_o[layer],
                                      attn_gain[layer], ffn_gain[layer])
            x_rows = ffn(h_rows, x_mid, w_gate[layer], w_up[layer], w_down[layer])
        return x_rows

    return jax.shard_map(device_fn, mesh=mesh, in_specs=in_specs, out_specs=out_specs, check_vma=False)
```

```python
import functools

import jax
import jax.numpy as jnp
import numpy as np
from jax import lax
from jax.experimental import pallas as pl
from jax.experimental.pallas import tpu as pltpu
from jax.sharding import PartitionSpec as P

EPS = 1e-5
ROPE_BASE = 10000.0
TILE = 512
SLOTS = 8
SEQS = 16
KV_BUFS = 4
VMEM_LIMIT = 66_000_000
MESH = pl.DeviceIdType.MESH


def rope_tables(cache, head):
    half = head // 2
    freqs = np.power(np.float32(ROPE_BASE), -np.arange(half, dtype=np.float32) / np.float32(half))
    angle = np.arange(cache + 1, dtype=np.float32)[:, None] * freqs.astype(np.float32)
    cos_part, sin_part = np.cos(angle.astype(np.float64)), np.sin(angle.astype(np.float64))
    cos_full = np.concatenate([cos_part, cos_part], axis=-1).astype(np.float32)
    sin_full = np.concatenate([-sin_part, sin_part], axis=-1).astype(np.float32)
    return cos_full[:, None], sin_full[:, None]


def layer_kernel(rows, len_ref, cos_tab, sin_tab, gain_ref, ffn_gain_ref, x_hbm, k_hbm, v_hbm, wq_hbm, wkv_hbm, wo_hbm,
                 wg_hbm, wu_hbm, wd_hbm, out_ref, ring, kv_buf, x_s, a_s, cos_s, sin_s, q_s, kv_s, ob_s, s_s, p_s,
                 tq, tx, tb, take_s, x1_s, h_all, u_s, part, recv, x_sem, w_sem, kv_sem, give_sem, take_sem,
                 h_send, h_recv, p_send, p_recv):
    width = x_hbm.shape[1]
    _, kv_heads, cache, head = k_hbm.shape
    kv_heads //= 2
    q_cols = wq_hbm.shape[1] // 2
    heads = q_cols // head
    group = heads // kv_heads
    pair = 2 * rows
    n_groups = pair // SEQS
    depth = wd_hbm.shape[0]
    n_q = q_cols // TILE
    n_col = width // TILE
    n_ff = depth // TILE
    o_first = n_q + 2
    ff_first = o_first + n_col
    per_pass = 2 * n_ff + n_col
    n_tiles = ff_first + 2 * per_pass

    side = lax.axis_index('side')
    core = lax.rem(side, 2)
    partner = side + 1 - 2 * core
    base = (side // 2) * pair
    dev = lax.axis_index('dev')
    flip = dev >= 2
    is_end = (dev == 0) | (dev == 3)
    is_mid = (dev == 1) | (dev == 2)
    end_dev = jnp.where(flip, 3, 0)
    mid_dev = jnp.where(flip, 2, 1)
    far_dev = jnp.where(flip, 1, 2)

    def column_copy(hbm, first_row, n_rows, first_col, slot):
        cols = pl.ds(pl.multiple_of(first_col, TILE), TILE)
        return pltpu.make_async_copy(hbm.at[pl.ds(first_row, n_rows), cols], ring.at[slot, pl.ds(0, n_rows)],
                                     w_sem.at[slot])

    def q_copy(t, slot):
        return column_copy(wq_hbm, 0, width, core * q_cols + t * TILE, slot)

    def kv_copy(which, slot):
        return column_copy(wkv_hbm, 0, width, (2 * which + core) * TILE, slot)

    def o_copy(t, slot):
        return column_copy(wo_hbm, core * q_cols, q_cols, t * TILE, slot)

    def gate_copy(t, slot):
        return column_copy(wg_hbm, 0, width, t * TILE, slot)

    def up_copy(t, slot):
        return column_copy(wu_hbm, 0, width, t * TILE, slot)

    def down_copy(t, slot):
        return column_copy(wd_hbm, 0, depth, t * TILE, slot)

    def start_ff(i):
        slot = lax.rem(i, SLOTS)
        r = lax.rem(i - ff_first, per_pass)
        live = i < n_tiles

        @pl.when(live & (r < 2 * n_ff) & (lax.rem(r, 2) == 0))
        def _():
            gate_copy(r // 2, slot).start()

        @pl.when(live & (r < 2 * n_ff) & (lax.rem(r, 2) == 1))
        def _():
            up_copy(r // 2, slot).start()

        @pl.when(live & (r >= 2 * n_ff))
        def _():
            down_copy(r - 2 * n_ff, slot).start()

    def each_kv(i, act):
        buf = lax.rem(i, KV_BUFS)
        at = (pl.ds(base + lax.rem(i, n_groups) * SEQS, SEQS), pl.ds(core * kv_heads, kv_heads))

        @pl.when(i < n_groups)
        def _():
            act(pltpu.make_async_copy(k_hbm.at[at], kv_buf.at[buf], kv_sem.at[buf]))

        @pl.when((i >= n_groups) & (i < 2 * n_groups))
        def _():
            act(pltpu.make_async_copy(v_hbm.at[at], kv_buf.at[buf], kv_sem.at[buf]))

    def start_kv(i):
        each_kv(i, lambda copy: copy.start())

    def wait_kv(i):
        each_kv(i, lambda copy: copy.wait())

    x_copy = pltpu.make_async_copy(x_hbm.at[pl.ds(base, pair)], x_s, x_sem)
    x_copy.start()
    for t in range(n_q):
        q_copy(t, t).start()
    for which in range(2):
        kv_copy(which, n_q + which).start()
    for i in range(KV_BUFS):
        start_kv(i)
    for t in range(SLOTS - o_first):
        o_copy(t, o_first + t).start()

    def signal(target):
        pl.semaphore_signal(pltpu.get_barrier_semaphore(), inc=1, device_id=target, device_id_type=MESH)

    signal({'side': partner})

    @pl.when(is_end)
    def _():
        signal({'dev': mid_dev})
        pl.semaphore_wait(pltpu.get_barrier_semaphore(), 2)

    @pl.when(is_mid)
    def _():
        signal({'dev': end_dev})
        signal({'dev': far_dev})
        pl.semaphore_wait(pltpu.get_barrier_semaphore(), 3)


    def lookup(i, carry):
        n = len_ref[base + i]
        cos_s[pl.ds(i, 1), :] = cos_tab[n]
        sin_s[pl.ds(i, 1), :] = sin_tab[n]
        return carry

    lax.fori_loop(0, pair, lookup, 0)
    x_copy.wait()
    x_f = x_s[...].astype(jnp.float32)
    inv = lax.rsqrt(jnp.mean(x_f * x_f, axis=-1, keepdims=True) + EPS)
    a_s[...] = (x_f * inv * gain_ref[...]).astype(jnp.bfloat16)

    def rotated(tile, i):
        vec = tile[:, i * head:(i + 1) * head]
        return vec * cos_s[...] + pltpu.roll(vec, head // 2, 1) * sin_s[...]

    def q_step(t, carry):
        q_copy(t, t).wait()
        tile = jnp.dot(a_s[...], ring[t], preferred_element_type=jnp.float32)
        for i in range(TILE // head):
            q_s[:, pl.ds(pl.multiple_of(t * TILE + i * head, head), head)] = rotated(tile, i)
        o_copy(t + SLOTS - o_first, t).start()
        return carry

    lax.fori_loop(0, n_q, q_step, 0)
    kv_copy(0, n_q).wait()
    tile = jnp.dot(a_s[...], ring[n_q], preferred_element_type=jnp.float32)
    for i in range(TILE // head):
        kv_s[:, i * head:(i + 1) * head] = rotated(tile, i)
    o_copy(n_col - 2, n_q).start()
    kv_copy(1, n_q + 1).wait()
    kv_s[:, TILE:] = jnp.dot(a_s[...], ring[n_q + 1], preferred_element_type=jnp.float32)
    o_copy(n_col - 1, n_q + 1).start()

    scale = head ** -0.5
    keys = kv_heads * cache
    row_head = lax.broadcasted_iota(jnp.int32, (heads, keys), 0) // group
    col = lax.broadcasted_iota(jnp.int32, (heads, keys), 1)
    key_pos = jnp.where(col // cache == row_head, col % cache, cache + 1)
    nt = (((1,), (1,)), ((), ()))

    def seq_rows(i):
        return pl.ds(pl.multiple_of(i * heads, heads), heads)

    def group_rows(g):
        return pl.ds(pl.multiple_of(g * SEQS, SEQS), SEQS)

    def spread_heads(g, first_col):
        for h in range(heads):
            at = first_col + (h // group) * head
            tx[pl.ds(h, SEQS, stride=heads), :] = kv_s[group_rows(g), at:at + head]
        return tx[...].astype(jnp.bfloat16).astype(jnp.float32)

    def score_group(g, carry):
        buf = lax.rem(g, KV_BUFS)
        for h in range(heads):
            tq[pl.ds(h, SEQS, stride=heads), :] = q_s[group_rows(g), h * head:(h + 1) * head]
        q = tq[...].astype(jnp.bfloat16)
        tb[...] = q
        s_own = jnp.sum(q.astype(jnp.float32) * spread_heads(g, 0), axis=-1, keepdims=True) * scale
        s_s[g, :, keys:] = jnp.broadcast_to(s_own, (SEQS * heads, head))
        wait_kv(g)

        def one(i, carry):
            k = kv_buf[buf, i].reshape(keys, head)
            s_s[g, seq_rows(i), :keys] = lax.dot_general(tb[seq_rows(i), :], k, nt, preferred_element_type=jnp.float32)
            return carry

        lax.fori_loop(0, SEQS, one, 0, unroll=True)
        start_kv(g + KV_BUFS)
        return carry

    def softmax_group(g, carry):
        def one(i, carry):
            n = len_ref[base + g * SEQS + i]
            s = jnp.where(key_pos < n, s_s[g, seq_rows(i), :keys] * scale, -1e30)
            s_own = s_s[g, seq_rows(i), keys:]
            top = jnp.maximum(jnp.max(s, axis=-1, keepdims=True), s_own)
            e = jnp.exp(s - top[:, :1])
            e_own = jnp.exp(s_own - top)
            p_s[g, seq_rows(i), :] = e.astype(jnp.bfloat16)
            s_s[g, seq_rows(i), :head] = jnp.sum(e, axis=-1, keepdims=True) + e_own
            s_s[g, seq_rows(i), keys:] = e_own.astype(jnp.bfloat16).astype(jnp.float32)
            return carry

        lax.fori_loop(0, SEQS, one, 0, unroll=True)
        return carry

    def mix_group(g, carry):
        buf = lax.rem(n_groups + g, KV_BUFS)
        wait_kv(n_groups + g)

        def one(i, carry):
            v = kv_buf[buf, i].reshape(keys, head)
            tq[seq_rows(i), :] = jnp.dot(p_s[g, seq_rows(i), :], v, preferred_element_type=jnp.float32)
            return carry

        lax.fori_loop(0, SEQS, one, 0, unroll=True)
        start_kv(n_groups + g + KV_BUFS)
        tq[...] = (tq[...] + s_s[g, :, keys:] * spread_heads(g, TILE)) / s_s[g, :, :head]
        for h in range(heads):
            q_s[group_rows(g), h * head:(h + 1) * head] = tq[pl.ds(h, SEQS, stride=heads), :]
        return carry

    lax.fori_loop(0, n_groups, score_group, 0)
    lax.fori_loop(0, n_groups, softmax_group, 0)
    lax.fori_loop(0, n_groups, mix_group, 0)
    ob_s[...] = q_s[...].astype(jnp.bfloat16)

    def give(t):
        return pltpu.make_async_remote_copy(
            src_ref=part.at[1, t], dst_ref=take_s.at[t], send_sem=give_sem.at[t], recv_sem=take_sem.at[t],
            device_id={'side': partner}, device_id_type=MESH)

    def o_step(t, carry):
        slot = lax.rem(o_first + t, SLOTS)
        o_copy(t, slot).wait()
        y = jnp.dot(ob_s[...], ring[slot, :q_cols], preferred_element_type=jnp.float32)
        part[1, t] = jnp.where(core == 0, y[rows:], y[:rows])
        give(t).start()
        part[0, t] = jnp.where(core == 0, y[:rows], y[rows:])
        start_ff(ff_first - o_first + o_first + t)
        return carry

    lax.fori_loop(0, n_col, o_step, 0)
    own_rows = pl.ds(pl.multiple_of(core * rows, rows), rows)

    def x1_step(t, square):
        give(t).wait_recv()
        give(t).wait_send()
        cols = pl.ds(pl.multiple_of(t * TILE, TILE), TILE)
        x1 = (x_s[own_rows, cols].astype(jnp.float32) + (part[0, t] + take_s[t])).astype(jnp.bfloat16)
        x1_s[:, cols] = x1
        x1_f = x1.astype(jnp.float32)
        return square + jnp.sum(x1_f * x1_f, axis=-1, keepdims=True)

    square = lax.fori_loop(0, n_col, x1_step, jnp.zeros((rows, 1), jnp.float32))
    inv = lax.rsqrt(square / width + EPS)
    me = jnp.where(is_end, 0, 1)
    h_all[me] = (x1_s[...].astype(jnp.float32) * inv * ffn_gain_ref[...]).astype(jnp.bfloat16)

    def send_h(src, dst, k, target):
        return pltpu.make_async_remote_copy(
            src_ref=h_all.at[src], dst_ref=h_all.at[dst], send_sem=h_send.at[k], recv_sem=h_recv.at[dst],
            device_id={'dev': target}, device_id_type=MESH)

    def send_part(j, c, slot, target):
        return pltpu.make_async_remote_copy(
            src_ref=part.at[j, c], dst_ref=recv.at[slot, c], send_sem=p_send.at[j, c], recv_sem=p_recv.at[slot, c],
            device_id={'dev': target}, device_id_type=MESH)

    @pl.when(is_end)
    def _():
        send_h(0, 0, 0, mid_dev).start()
        send_h(0, 1, 0, mid_dev).wait_recv()

    @pl.when(is_mid)
    def _():
        send_h(1, 1, 0, end_dev).start()
        send_h(1, 2, 1, far_dev).start()
        send_h(1, 0, 0, end_dev).wait_recv()
        send_h(0, 3, 2, far_dev).start()
        send_h(1, 2, 0, end_dev).wait_recv()
        send_h(2, 2, 3, end_dev).start()

    for half in range(2):
        def ff_step(t, carry):
            i = ff_first + half * per_pass + 2 * t
            slot_g, slot_u = lax.rem(i, SLOTS), lax.rem(i + 1, SLOTS)
            h = h_all[2 * half:2 * half + 2].reshape(2 * rows, width)
            gate_copy(t, slot_g).wait()
            gate = jnp.dot(h, ring[slot_g], preferred_element_type=jnp.float32)
            start_ff(i + SLOTS)
            up_copy(t, slot_u).wait()
            up = jnp.dot(h, ring[slot_u], preferred_element_type=jnp.float32)
            start_ff(i + 1 + SLOTS)
            u_s[:, pl.ds(pl.multiple_of(t * TILE, TILE), TILE)] = (jax.nn.silu(gate) * up).astype(jnp.bfloat16)
            return carry

        def down_step(c, carry):
            i = ff_first + half * per_pass + 2 * n_ff + c
            slot = lax.rem(i, SLOTS)
            down_copy(c, slot).wait()
            y = jnp.dot(u_s[...], ring[slot, :depth], preferred_element_type=jnp.float32)
            start_ff(i + SLOTS)
            part[2 * half, c] = y[:rows]
            part[2 * half + 1, c] = y[rows:]

            @pl.when(is_end)
            def _():
                send_part(2 * half + 1, c, 2 * half, mid_dev).start()

            if half == 0:
                @pl.when(is_mid & (c == n_col - 3))
                def _():
                    send_h(1, 3, 0, end_dev).wait_recv()
                    send_h(3, 3, 4, end_dev).start()

            return carry

        if half == 1:
            @pl.when(is_end)
            def _():
                send_h(0, 2, 0, mid_dev).wait_recv()
                send_h(0, 3, 0, mid_dev).wait_recv()

        lax.fori_loop(0, n_ff, ff_step, 0)
        lax.fori_loop(0, n_col, down_step, 0)

    def finish(c, y):
        cols = pl.ds(pl.multiple_of(c * TILE, TILE), TILE)
        y = y.astype(jnp.bfloat16).astype(jnp.float32)
        out_ref[:, cols] = (x1_s[:, cols].astype(jnp.float32) + y).astype(jnp.bfloat16)

    @pl.when(is_end)
    def _():
        def second(c, carry):
            send_part(2, c, 1, mid_dev).start()
            return carry

        def home(c, carry):
            send_part(0, c, 0, mid_dev).wait_recv()
            finish(c, part[0, c] + recv[0, c])
            return carry

        def drain(c, carry):
            for j in (1, 3, 2):
                send_part(j, c, 0, mid_dev).wait_send()
            return carry

        lax.fori_loop(0, n_col, second, 0)
        lax.fori_loop(0, n_col, home, 0)
        lax.fori_loop(0, n_col, drain, 0)
        send_h(0, 0, 0, mid_dev).wait_send()

    @pl.when(is_mid)
    def _():
        def back(c):
            send_part(0, c, 4, far_dev).wait_recv()
            part[0, c] += recv[4, c]
            send_part(0, c, 0, end_dev).start()

        def across(c, carry):
            send_part(3, c, 2, end_dev).wait_recv()
            part[3, c] += recv[2, c]
            send_part(3, c, 4, far_dev).start()

            @pl.when(c > 0)
            def _():
                back(c - 1)

            return carry

        def home(c):
            send_part(1, c, 0, end_dev).wait_recv()
            send_part(1, c, 3, far_dev).wait_recv()
            finish(c, part[1, c] + recv[0, c] + recv[3, c])

        def near(c, carry):
            send_part(2, c, 1, end_dev).wait_recv()
            part[2, c] += recv[1, c]
            send_part(2, c, 3, far_dev).start()

            @pl.when(c > 0)
            def _():
                home(c - 1)

            return carry

        def drain(c, carry):
            for j in (3, 0, 2):
                send_part(j, c, 0, far_dev).wait_send()
            return carry

        lax.fori_loop(0, n_col, across, 0)
        back(n_col - 1)
        lax.fori_loop(0, n_col, near, 0)
        home(n_col - 1)
        lax.fori_loop(0, n_col, drain, 0)
        for k in range(5):
            send_h(0, 0, k, end_dev).wait_send()


def layer_step(hidden, lengths, k_cache, v_cache, w_q, w_kv, w_o, gain_attn, gain_ffn, w_gate, w_up, w_down, n_side):
    rows, width = hidden.shape[0] // n_side, hidden.shape[1]
    _, kv_heads, cache, head = k_cache.shape
    q_cols = w_q.shape[1] // 2
    heads = q_cols // head
    depth = w_down.shape[0]
    n_col = width // TILE
    assert kv_heads * head == 2 * TILE, "tile"
    cos_tab, sin_tab = rope_tables(cache, head)
    vmem = pl.BlockSpec(memory_space=pltpu.VMEM)
    hbm = pl.BlockSpec(memory_space=pl.ANY)
    f32, bf16 = jnp.float32, jnp.bfloat16
    dma = pltpu.SemaphoreType.DMA
    kv_block = (KV_BUFS, SEQS, kv_heads // 2, cache, head)
    return pl.pallas_call(
        functools.partial(layer_kernel, rows),
        out_shape=jax.ShapeDtypeStruct((rows, width), bf16),
        in_specs=[pl.BlockSpec(memory_space=pltpu.SMEM)] + [vmem] * 4 + [hbm] * 9,
        out_specs=vmem,
        scratch_shapes=[
            pltpu.VMEM((SLOTS, width, TILE), bf16),
            pltpu.VMEM(kv_block, bf16),
            pltpu.VMEM((2 * rows, width), bf16),
            pltpu.VMEM((2 * rows, width), bf16),
            pltpu.VMEM((2 * rows, head), f32),
            pltpu.VMEM((2 * rows, head), f32),
            pltpu.VMEM((2 * rows, q_cols), f32),
            pltpu.VMEM((2 * rows, 2 * TILE), f32),
            pltpu.VMEM((2 * rows, q_cols), bf16),
            pltpu.VMEM((2 * rows // SEQS, SEQS * heads, kv_heads // 2 * cache + head), f32),
            pltpu.VMEM((2 * rows // SEQS, SEQS * heads, kv_heads // 2 * cache), bf16),
            pltpu.VMEM((SEQS * heads, head), f32),
            pltpu.VMEM((SEQS * heads, head), f32),
            pltpu.VMEM((SEQS * heads, head), bf16),
            pltpu.VMEM((n_col, rows, TILE), f32),
            pltpu.VMEM((rows, width), bf16),
            pltpu.VMEM((4, rows, width), bf16),
            pltpu.VMEM((2 * rows, depth), bf16),
            pltpu.VMEM((4, n_col, rows, TILE), f32),
            pltpu.VMEM((5, n_col, rows, TILE), f32),
            dma(()),
            dma((SLOTS,)),
            dma((KV_BUFS,)),
            dma((n_col,)),
            dma((n_col,)),
            dma((5,)),
            dma((4,)),
            dma((4, n_col)),
            dma((5, n_col)),
        ],
        compiler_params=pltpu.CompilerParams(vmem_limit_bytes=VMEM_LIMIT, collective_id=0, has_side_effects=True),
        name="layer",
    )(lengths, jnp.asarray(cos_tab), jnp.asarray(sin_tab), gain_attn[None], gain_ffn[None], hidden, k_cache, v_cache,
      w_q, w_kv, w_o, w_gate, w_up, w_down)


def solution(mesh):
    n_side = mesh.shape['side']
    assert n_side == 4 and mesh.shape['dev'] == 4, "mesh"
    batch_axes = ('inst', 'dev')
    in_specs = (
        P(batch_axes, None),
        P(batch_axes),
        P(None, batch_axes, None, None, None),
        P(None, batch_axes, None, None, None),
        P(), P(), P(), P(), P(),
        P(None, None, 'dev'),
        P(None, None, 'dev'),
        P(None, 'dev', None),
    )
    out_specs = P(('inst', 'dev', 'side'), None)

    def device_fn(hidden, cache_len, k_cache, v_cache, w_q, w_kv, w_o, attn_gain, ffn_gain, w_gate, w_up, w_down):
        assert w_q.shape[0] == 1, "layers"
        return layer_step(hidden, cache_len, k_cache[0], v_cache[0], w_q[0], w_kv[0], w_o[0], attn_gain[0], ffn_gain[0],
                          w_gate[0], w_up[0], w_down[0], n_side)

    return jax.shard_map(device_fn, mesh=mesh, in_specs=in_specs, out_specs=out_specs, check_vma=False)
```

```python
import functools

import jax
import jax.numpy as jnp
import numpy as np
from jax import lax
from jax.experimental import pallas as pl
from jax.experimental.pallas import tpu as pltpu
from jax.sharding import PartitionSpec as P

EPS = 1e-5
ROPE_BASE = 10000.0
TILE = 512
SLOTS = 8
SEQS = 16
KV_BUFS = 12
FFN_SLOTS = 10
VMEM_LIMIT = 66_000_000
MESH = pl.DeviceIdType.MESH


def rope_tables(cache, head):
    half = head // 2
    freqs = np.power(np.float32(ROPE_BASE), -np.arange(half, dtype=np.float32) / np.float32(half))
    angle = np.arange(cache + 1, dtype=np.float32)[:, None] * freqs.astype(np.float32)
    cos_part, sin_part = np.cos(angle.astype(np.float64)), np.sin(angle.astype(np.float64))
    cos_full = np.concatenate([cos_part, cos_part], axis=-1).astype(np.float32)
    sin_full = np.concatenate([-sin_part, sin_part], axis=-1).astype(np.float32)
    return cos_full[:, None], sin_full[:, None]


def attention_kernel(rows, len_ref, cos_tab, sin_tab, gain_ref, x_hbm, k_hbm, v_hbm, wq_hbm, wkv_hbm, wo_hbm, own_ref,
                     give_ref, ring, kv_buf, x_s, a_s, cos_s, sin_s, q_s, kv_s, ob_s, s_s, p_s, tq, tx, tb, x_sem, w_sem,
                     kv_sem):
    width = x_hbm.shape[1]
    _, kv_heads, cache, head = k_hbm.shape
    kv_heads //= 2
    q_cols = wq_hbm.shape[1] // 2
    heads = q_cols // head
    group = heads // kv_heads
    pair = 2 * rows
    n_groups = pair // SEQS
    n_q = q_cols // TILE
    n_col = width // TILE
    o_first = n_q + 2

    side = lax.axis_index('side')
    core = lax.rem(side, 2)
    base = (side // 2) * pair

    def column_copy(hbm, first_row, n_rows, first_col, slot):
        cols = pl.ds(pl.multiple_of(first_col, TILE), TILE)
        return pltpu.make_async_copy(hbm.at[pl.ds(first_row, n_rows), cols], ring.at[slot, pl.ds(0, n_rows)],
                                     w_sem.at[slot])

    def q_copy(t, slot):
        return column_copy(wq_hbm, 0, width, core * q_cols + t * TILE, slot)

    def kv_copy(which, slot):
        return column_copy(wkv_hbm, 0, width, (2 * which + core) * TILE, slot)

    def o_copy(t, slot):
        return column_copy(wo_hbm, core * q_cols, q_cols, t * TILE, slot)

    def each_kv(i, act):
        buf = lax.rem(i, KV_BUFS)
        at = (pl.ds(base + lax.rem(i, n_groups) * SEQS, SEQS), pl.ds(core * kv_heads, kv_heads))

        @pl.when(i < n_groups)
        def _():
            act(pltpu.make_async_copy(k_hbm.at[at], kv_buf.at[buf], kv_sem.at[buf]))

        @pl.when((i >= n_groups) & (i < 2 * n_groups))
        def _():
            act(pltpu.make_async_copy(v_hbm.at[at], kv_buf.at[buf], kv_sem.at[buf]))

    def start_kv(i):
        each_kv(i, lambda copy: copy.start())

    def wait_kv(i):
        each_kv(i, lambda copy: copy.wait())

    x_copy = pltpu.make_async_copy(x_hbm.at[pl.ds(base, pair)], x_s, x_sem)
    x_copy.start()
    for t in range(n_q):
        q_copy(t, t).start()
    for which in range(2):
        kv_copy(which, n_q + which).start()
    for i in range(KV_BUFS):
        start_kv(i)
    for t in range(SLOTS - o_first):
        o_copy(t, o_first + t).start()

    def lookup(i, carry):
        n = len_ref[base + i]
        cos_s[pl.ds(i, 1), :] = cos_tab[n]
        sin_s[pl.ds(i, 1), :] = sin_tab[n]
        return carry

    lax.fori_loop(0, pair, lookup, 0, unroll=8)
    x_copy.wait()
    x_f = x_s[...].astype(jnp.float32)
    inv = lax.rsqrt(jnp.mean(x_f * x_f, axis=-1, keepdims=True) + EPS)
    a_s[...] = (x_f * inv * gain_ref[...]).astype(jnp.bfloat16)

    def rotated(tile, i):
        vec = tile[:, i * head:(i + 1) * head]
        return vec * cos_s[...] + pltpu.roll(vec, head // 2, 1) * sin_s[...]

    def q_step(t, carry):
        q_copy(t, t).wait()
        tile = jnp.dot(a_s[...], ring[t], preferred_element_type=jnp.float32)
        for i in range(TILE // head):
            q_s[:, pl.ds(pl.multiple_of(t * TILE + i * head, head), head)] = rotated(tile, i)
        o_copy(t + SLOTS - o_first, t).start()
        return carry

    lax.fori_loop(0, n_q, q_step, 0)
    kv_copy(0, n_q).wait()
    tile = jnp.dot(a_s[...], ring[n_q], preferred_element_type=jnp.float32)
    for i in range(TILE // head):
        kv_s[:, i * head:(i + 1) * head] = rotated(tile, i)
    o_copy(n_col - 2, n_q).start()
    kv_copy(1, n_q + 1).wait()
    kv_s[:, TILE:] = jnp.dot(a_s[...], ring[n_q + 1], preferred_element_type=jnp.float32)
    o_copy(n_col - 1, n_q + 1).start()

    scale = head ** -0.5
    keys = kv_heads * cache
    row_head = lax.broadcasted_iota(jnp.int32, (heads, keys), 0) // group
    col = lax.broadcasted_iota(jnp.int32, (heads, keys), 1)
    key_pos = jnp.where(col // cache == row_head, col % cache, cache + 1)
    nt = (((1,), (1,)), ((), ()))

    def seq_rows(i):
        return pl.ds(pl.multiple_of(i * heads, heads), heads)

    def group_rows(g):
        return pl.ds(pl.multiple_of(g * SEQS, SEQS), SEQS)

    def spread_heads(g, first_col):
        for h in range(heads):
            at = first_col + (h // group) * head
            tx[pl.ds(h, SEQS, stride=heads), :] = kv_s[group_rows(g), at:at + head]
        return tx[...].astype(jnp.bfloat16).astype(jnp.float32)

    def score_group(g, carry):
        buf = lax.rem(g, KV_BUFS)
        for h in range(heads):
            tq[pl.ds(h, SEQS, stride=heads), :] = q_s[group_rows(g), h * head:(h + 1) * head]
        q = tq[...].astype(jnp.bfloat16)
        tb[...] = q
        s_own = jnp.sum(q.astype(jnp.float32) * spread_heads(g, 0), axis=-1, keepdims=True) * scale
        s_s[g, :, keys:] = jnp.broadcast_to(s_own, (SEQS * heads, head))
        wait_kv(g)

        def one(i, carry):
            k = kv_buf[buf, i].reshape(keys, head)
            s_s[g, seq_rows(i), :keys] = lax.dot_general(tb[seq_rows(i), :], k, nt, preferred_element_type=jnp.float32)
            return carry

        lax.fori_loop(0, SEQS, one, 0, unroll=True)
        start_kv(g + KV_BUFS)
        return carry

    def softmax_group(g, carry):
        def one(i, carry):
            n = len_ref[base + g * SEQS + i]
            s = jnp.where(key_pos < n, s_s[g, seq_rows(i), :keys] * scale, -1e30)
            s_own = s_s[g, seq_rows(i), keys:]
            top = jnp.maximum(jnp.max(s, axis=-1, keepdims=True), s_own)
            e = jnp.exp(s - top[:, :1])
            e_own = jnp.exp(s_own - top)
            p_s[g, seq_rows(i), :] = e.astype(jnp.bfloat16)
            s_s[g, seq_rows(i), :head] = jnp.sum(e, axis=-1, keepdims=True) + e_own
            s_s[g, seq_rows(i), keys:] = e_own.astype(jnp.bfloat16).astype(jnp.float32)
            return carry

        lax.fori_loop(0, SEQS, one, 0, unroll=True)
        return carry

    def mix_group(g, carry):
        buf = lax.rem(n_groups + g, KV_BUFS)
        wait_kv(n_groups + g)

        def one(i, carry):
            v = kv_buf[buf, i].reshape(keys, head)
            tq[seq_rows(i), :] = jnp.dot(p_s[g, seq_rows(i), :], v, preferred_element_type=jnp.float32)
            return carry

        lax.fori_loop(0, SEQS, one, 0, unroll=True)
        start_kv(n_groups + g + KV_BUFS)
        tq[...] = (tq[...] + s_s[g, :, keys:] * spread_heads(g, TILE)) / s_s[g, :, :head]
        for h in range(heads):
            q_s[group_rows(g), h * head:(h + 1) * head] = tq[pl.ds(h, SEQS, stride=heads), :]
        return carry

    lax.fori_loop(0, n_groups, score_group, 0)
    lax.fori_loop(0, n_groups, softmax_group, 0)
    lax.fori_loop(0, n_groups, mix_group, 0)
    ob_s[...] = q_s[...].astype(jnp.bfloat16)

    own_rows = pl.ds(pl.multiple_of(core * rows, rows), rows)

    def o_step(t, carry):
        slot = lax.rem(o_first + t, SLOTS)
        o_copy(t, slot).wait()
        y = jnp.dot(ob_s[...], ring[slot, :q_cols], preferred_element_type=jnp.float32)
        cols = pl.ds(pl.multiple_of(t * TILE, TILE), TILE)
        give_ref[t] = jnp.where(core == 0, y[rows:], y[:rows])
        own_ref[t] = jnp.where(core == 0, y[:rows], y[rows:]) + x_s[own_rows, cols].astype(jnp.float32)
        return carry

    lax.fori_loop(0, n_col, o_step, 0)


def ffn_kernel(own_ref, give_ref, ffn_gain_ref, wg_hbm, wu_hbm, wd_hbm, out_ref, ring, take_s, x1_s, h_all, u_s, part, recv,
               w_sem, give_sem, take_sem, h_send, h_recv, p_send, p_recv):
    rows, width = x1_s.shape
    depth = wd_hbm.shape[0]
    n_col = width // TILE
    n_ff = depth // TILE
    per_pass = 2 * n_ff + n_col
    n_tiles = 2 * per_pass

    side = lax.axis_index('side')
    partner = side + 1 - 2 * lax.rem(side, 2)
    dev = lax.axis_index('dev')
    flip = dev >= 2
    is_end = (dev == 0) | (dev == 3)
    is_mid = (dev == 1) | (dev == 2)
    end_dev = jnp.where(flip, 3, 0)
    mid_dev = jnp.where(flip, 2, 1)
    far_dev = jnp.where(flip, 1, 2)

    def column_copy(hbm, first_row, n_rows, first_col, slot):
        cols = pl.ds(pl.multiple_of(first_col, TILE), TILE)
        return pltpu.make_async_copy(hbm.at[pl.ds(first_row, n_rows), cols], ring.at[slot, pl.ds(0, n_rows)],
                                     w_sem.at[slot])

    def gate_copy(t, slot):
        return column_copy(wg_hbm, 0, width, t * TILE, slot)

    def up_copy(t, slot):
        return column_copy(wu_hbm, 0, width, t * TILE, slot)

    def down_copy(t, slot):
        return column_copy(wd_hbm, 0, depth, t * TILE, slot)

    def start_ff(i):
        slot = lax.rem(i, FFN_SLOTS)
        r = lax.rem(i, per_pass)
        live = i < n_tiles

        @pl.when(live & (r < 2 * n_ff) & (lax.rem(r, 2) == 0))
        def _():
            gate_copy(r // 2, slot).start()

        @pl.when(live & (r < 2 * n_ff) & (lax.rem(r, 2) == 1))
        def _():
            up_copy(r // 2, slot).start()

        @pl.when(live & (r >= 2 * n_ff))
        def _():
            down_copy(r - 2 * n_ff, slot).start()

    def first(i, carry):
        start_ff(i)
        return carry

    lax.fori_loop(0, FFN_SLOTS, first, 0)

    def signal(target):
        pl.semaphore_signal(pltpu.get_barrier_semaphore(), inc=1, device_id=target, device_id_type=MESH)

    signal({'side': partner})

    @pl.when(is_end)
    def _():
        signal({'dev': mid_dev})
        pl.semaphore_wait(pltpu.get_barrier_semaphore(), 2)

    @pl.when(is_mid)
    def _():
        signal({'dev': end_dev})
        signal({'dev': far_dev})
        pl.semaphore_wait(pltpu.get_barrier_semaphore(), 3)


    def give(t):
        return pltpu.make_async_remote_copy(
            src_ref=give_ref.at[t], dst_ref=take_s.at[t], send_sem=give_sem.at[t], recv_sem=take_sem.at[t],
            device_id={'side': partner}, device_id_type=MESH)

    def give_step(t, carry):
        give(t).start()
        return carry

    lax.fori_loop(0, n_col, give_step, 0)

    def x1_step(t, square):
        give(t).wait_recv()
        give(t).wait_send()
        cols = pl.ds(pl.multiple_of(t * TILE, TILE), TILE)
        x1 = (own_ref[t] + take_s[t]).astype(jnp.bfloat16)
        x1_s[:, cols] = x1
        x1_f = x1.astype(jnp.float32)
        return square + jnp.sum(x1_f * x1_f, axis=-1, keepdims=True)

    square = lax.fori_loop(0, n_col, x1_step, jnp.zeros((rows, 1), jnp.float32))
    inv = lax.rsqrt(square / width + EPS)
    me = jnp.where(is_end, 0, 1)
    h_all[me] = (x1_s[...].astype(jnp.float32) * inv * ffn_gain_ref[...]).astype(jnp.bfloat16)

    def send_h(src, dst, k, target):
        return pltpu.make_async_remote_copy(
            src_ref=h_all.at[src], dst_ref=h_all.at[dst], send_sem=h_send.at[k], recv_sem=h_recv.at[dst],
            device_id={'dev': target}, device_id_type=MESH)

    def send_part(j, c, slot, target):
        return pltpu.make_async_remote_copy(
            src_ref=part.at[j, c], dst_ref=recv.at[slot, c], send_sem=p_send.at[j, c], recv_sem=p_recv.at[slot, c],
            device_id={'dev': target}, device_id_type=MESH)

    @pl.when(is_end)
    def _():
        send_h(0, 0, 0, mid_dev).start()
        send_h(0, 1, 0, mid_dev).wait_recv()

    @pl.when(is_mid)
    def _():
        send_h(1, 1, 0, end_dev).start()
        send_h(1, 2, 1, far_dev).start()
        send_h(1, 0, 0, end_dev).wait_recv()
        send_h(0, 3, 2, far_dev).start()
        send_h(1, 2, 0, end_dev).wait_recv()
        send_h(2, 2, 3, end_dev).start()

    for half in range(2):
        def ff_step(t, carry):
            i = half * per_pass + 2 * t
            slot_g, slot_u = lax.rem(i, FFN_SLOTS), lax.rem(i + 1, FFN_SLOTS)
            h = h_all[2 * half:2 * half + 2].reshape(2 * rows, width)
            gate_copy(t, slot_g).wait()
            gate = jnp.dot(h, ring[slot_g], preferred_element_type=jnp.float32)
            start_ff(i + FFN_SLOTS)
            up_copy(t, slot_u).wait()
            up = jnp.dot(h, ring[slot_u], preferred_element_type=jnp.float32)
            start_ff(i + 1 + FFN_SLOTS)
            u_s[:, pl.ds(pl.multiple_of(t * TILE, TILE), TILE)] = (jax.nn.silu(gate) * up).astype(jnp.bfloat16)
            return carry

        def down_step(c, carry):
            i = half * per_pass + 2 * n_ff + c
            slot = lax.rem(i, FFN_SLOTS)
            down_copy(c, slot).wait()
            y = jnp.dot(u_s[...], ring[slot, :depth], preferred_element_type=jnp.float32)
            start_ff(i + FFN_SLOTS)
            part[2 * half, c] = y[:rows]
            part[2 * half + 1, c] = y[rows:]

            @pl.when(is_end)
            def _():
                send_part(2 * half + 1, c, 2 * half, mid_dev).start()

            if half == 0:
                @pl.when(is_mid & (c == n_col - 3))
                def _():
                    send_h(1, 3, 0, end_dev).wait_recv()
                    send_h(3, 3, 4, end_dev).start()

            return carry

        if half == 1:
            @pl.when(is_end)
            def _():
                send_h(0, 2, 0, mid_dev).wait_recv()
                send_h(0, 3, 0, mid_dev).wait_recv()

        lax.fori_loop(0, n_ff, ff_step, 0)
        lax.fori_loop(0, n_col, down_step, 0)

    def finish(c, y):
        cols = pl.ds(pl.multiple_of(c * TILE, TILE), TILE)
        y = y.astype(jnp.bfloat16).astype(jnp.float32)
        out_ref[:, cols] = (x1_s[:, cols].astype(jnp.float32) + y).astype(jnp.bfloat16)

    @pl.when(is_end)
    def _():
        def second(c, carry):
            send_part(2, c, 1, mid_dev).start()
            return carry

        def home(c, carry):
            send_part(0, c, 0, mid_dev).wait_recv()
            finish(c, part[0, c] + recv[0, c])
            return carry

        def drain(c, carry):
            for j in (1, 3, 2):
                send_part(j, c, 0, mid_dev).wait_send()
            return carry

        lax.fori_loop(0, n_col, second, 0)
        lax.fori_loop(0, n_col, home, 0)
        lax.fori_loop(0, n_col, drain, 0)
        send_h(0, 0, 0, mid_dev).wait_send()

    @pl.when(is_mid)
    def _():
        def back(c):
            send_part(0, c, 4, far_dev).wait_recv()
            part[0, c] += recv[4, c]
            send_part(0, c, 0, end_dev).start()

        def across(c, carry):
            send_part(3, c, 2, end_dev).wait_recv()
            part[3, c] += recv[2, c]
            send_part(3, c, 4, far_dev).start()

            @pl.when(c > 0)
            def _():
                back(c - 1)

            return carry

        def home(c):
            send_part(1, c, 0, end_dev).wait_recv()
            send_part(1, c, 3, far_dev).wait_recv()
            finish(c, part[1, c] + recv[0, c] + recv[3, c])

        def near(c, carry):
            send_part(2, c, 1, end_dev).wait_recv()
            part[2, c] += recv[1, c]
            send_part(2, c, 3, far_dev).start()

            @pl.when(c > 0)
            def _():
                home(c - 1)

            return carry

        def drain(c, carry):
            for j in (3, 0, 2):
                send_part(j, c, 0, far_dev).wait_send()
            return carry

        lax.fori_loop(0, n_col, across, 0)
        back(n_col - 1)
        lax.fori_loop(0, n_col, near, 0)
        home(n_col - 1)
        lax.fori_loop(0, n_col, drain, 0)
        for k in range(5):
            send_h(0, 0, k, end_dev).wait_send()


def attention(hidden, lengths, k_cache, v_cache, w_q, w_kv, w_o, gain, n_side):
    rows, width = hidden.shape[0] // n_side, hidden.shape[1]
    _, kv_heads, cache, head = k_cache.shape
    q_cols = w_q.shape[1] // 2
    heads = q_cols // head
    n_col = width // TILE
    keys = kv_heads // 2 * cache
    assert kv_heads * head == 2 * TILE, "tile"
    cos_tab, sin_tab = rope_tables(cache, head)
    vmem = pl.BlockSpec(memory_space=pltpu.VMEM)
    hbm = pl.BlockSpec(memory_space=pl.ANY)
    f32, bf16 = jnp.float32, jnp.bfloat16
    dma = pltpu.SemaphoreType.DMA
    partial = jax.ShapeDtypeStruct((n_col, rows, TILE), f32)
    return pl.pallas_call(
        functools.partial(attention_kernel, rows),
        out_shape=(partial, partial),
        in_specs=[pl.BlockSpec(memory_space=pltpu.SMEM)] + [vmem] * 3 + [hbm] * 6,
        out_specs=(vmem, vmem),
        scratch_shapes=[
            pltpu.VMEM((SLOTS, width, TILE), bf16),
            pltpu.VMEM((KV_BUFS, SEQS, kv_heads // 2, cache, head), bf16),
            pltpu.VMEM((2 * rows, width), bf16),
            pltpu.VMEM((2 * rows, width), bf16),
            pltpu.VMEM((2 * rows, head), f32),
            pltpu.VMEM((2 * rows, head), f32),
            pltpu.VMEM((2 * rows, q_cols), f32),
            pltpu.VMEM((2 * rows, 2 * TILE), f32),
            pltpu.VMEM((2 * rows, q_cols), bf16),
            pltpu.VMEM((2 * rows // SEQS, SEQS * heads, keys + head), f32),
            pltpu.VMEM((2 * rows // SEQS, SEQS * heads, keys), bf16),
            pltpu.VMEM((SEQS * heads, head), f32),
            pltpu.VMEM((SEQS * heads, head), f32),
            pltpu.VMEM((SEQS * heads, head), bf16),
            dma(()),
            dma((SLOTS,)),
            dma((KV_BUFS,)),
        ],
        compiler_params=pltpu.CompilerParams(vmem_limit_bytes=VMEM_LIMIT),
        name="attention",
    )(lengths, jnp.asarray(cos_tab), jnp.asarray(sin_tab), gain[None], hidden, k_cache, v_cache, w_q, w_kv, w_o)


def ffn(own, give, gain, w_gate, w_up, w_down):
    n_col, rows, _ = own.shape
    width = n_col * TILE
    depth = w_down.shape[0]
    vmem = pl.BlockSpec(memory_space=pltpu.VMEM)
    hbm = pl.BlockSpec(memory_space=pl.ANY)
    f32, bf16 = jnp.float32, jnp.bfloat16
    dma = pltpu.SemaphoreType.DMA
    return pl.pallas_call(
        ffn_kernel,
        out_shape=jax.ShapeDtypeStruct((rows, width), bf16),
        in_specs=[vmem] * 3 + [hbm] * 3,
        out_specs=vmem,
        scratch_shapes=[
            pltpu.VMEM((FFN_SLOTS, width, TILE), bf16),
            pltpu.VMEM((n_col, rows, TILE), f32),
            pltpu.VMEM((rows, width), bf16),
            pltpu.VMEM((4, rows, width), bf16),
            pltpu.VMEM((2 * rows, depth), bf16),
            pltpu.VMEM((4, n_col, rows, TILE), f32),
            pltpu.VMEM((5, n_col, rows, TILE), f32),
            dma((FFN_SLOTS,)),
            dma((n_col,)),
            dma((n_col,)),
            dma((5,)),
            dma((4,)),
            dma((4, n_col)),
            dma((5, n_col)),
        ],
        compiler_params=pltpu.CompilerParams(vmem_limit_bytes=VMEM_LIMIT, collective_id=0, has_side_effects=True),
        name="ffn",
    )(own, give, gain[None], w_gate, w_up, w_down)


def solution(mesh):
    n_side = mesh.shape['side']
    assert n_side == 4 and mesh.shape['dev'] == 4, "mesh"
    batch_axes = ('inst', 'dev')
    in_specs = (
        P(batch_axes, None),
        P(batch_axes),
        P(None, batch_axes, None, None, None),
        P(None, batch_axes, None, None, None),
        P(), P(), P(), P(), P(),
        P(None, None, 'dev'),
        P(None, None, 'dev'),
        P(None, 'dev', None),
    )
    out_specs = P(('inst', 'dev', 'side'), None)

    def device_fn(hidden, cache_len, k_cache, v_cache, w_q, w_kv, w_o, attn_gain, ffn_gain, w_gate, w_up, w_down):
        assert w_q.shape[0] == 1, "layers"
        own, give = attention(hidden, cache_len, k_cache[0], v_cache[0], w_q[0], w_kv[0], w_o[0], attn_gain[0], n_side)
        return ffn(own, give, ffn_gain[0], w_gate[0], w_up[0], w_down[0])

    return jax.shard_map(device_fn, mesh=mesh, in_specs=in_specs, out_specs=out_specs, check_vma=False)
```

```python
import functools

import jax
import jax.numpy as jnp
import numpy as np
from jax import lax
from jax.experimental import pallas as pl
from jax.experimental.pallas import tpu as pltpu
from jax.sharding import PartitionSpec as P

EPS = 1e-5
ROPE_BASE = 10000.0
TILE = 512
SLOTS = 8
SEQS = 16
KV_BUFS = 4
AHEAD = 3
VMEM_LIMIT = 66_000_000
MESH = pl.DeviceIdType.MESH


def rope_tables(cache, head):
    half = head // 2
    freqs = np.power(np.float32(ROPE_BASE), -np.arange(half, dtype=np.float32) / np.float32(half))
    angle = np.arange(cache + 1, dtype=np.float32)[:, None] * freqs.astype(np.float32)
    cos_part, sin_part = np.cos(angle.astype(np.float64)), np.sin(angle.astype(np.float64))
    cos_full = np.concatenate([cos_part, cos_part], axis=-1).astype(np.float32)
    sin_full = np.concatenate([-sin_part, sin_part], axis=-1).astype(np.float32)
    return cos_full[:, None], sin_full[:, None]


def layer_kernel(rows, len_ref, cos_tab, sin_tab, gain_ref, ffn_gain_ref, x_hbm, k_hbm, v_hbm, wq_hbm, wkv_hbm, wo_hbm,
                 wg_hbm, wu_hbm, wd_hbm, out_ref, ring, kv_buf, x_s, a_s, cos_s, sin_s, q_s, kv_s, ob_s, s_s, p_s,
                 tq, tx, tb, take_s, x1_s, h_all, u_s, part, recv, x_sem, w_sem, kv_sem, give_sem, take_sem,
                 h_send, h_recv, p_send, p_recv):
    width = x_hbm.shape[1]
    _, kv_heads, cache, head = k_hbm.shape
    kv_heads //= 2
    q_cols = wq_hbm.shape[1] // 2
    heads = q_cols // head
    group = heads // kv_heads
    pair = 2 * rows
    n_groups = pair // SEQS
    assert n_groups == width // TILE and q_cols // TILE == AHEAD + 1, "groups"
    depth = wd_hbm.shape[0]
    n_q = q_cols // TILE
    n_col = width // TILE
    n_ff = depth // TILE
    o_first = n_q + 2
    ff_first = o_first + n_col
    per_pass = 2 * n_ff + n_col
    n_tiles = ff_first + 2 * per_pass

    side = lax.axis_index('side')
    core = lax.rem(side, 2)
    partner = side + 1 - 2 * core
    base = (side // 2) * pair
    dev = lax.axis_index('dev')
    flip = dev >= 2
    is_end = (dev == 0) | (dev == 3)
    is_mid = (dev == 1) | (dev == 2)
    end_dev = jnp.where(flip, 3, 0)
    mid_dev = jnp.where(flip, 2, 1)
    far_dev = jnp.where(flip, 1, 2)

    def column_copy(hbm, first_row, n_rows, first_col, slot):
        cols = pl.ds(pl.multiple_of(first_col, TILE), TILE)
        return pltpu.make_async_copy(hbm.at[pl.ds(first_row, n_rows), cols], ring.at[slot, pl.ds(0, n_rows)],
                                     w_sem.at[slot])

    def q_copy(t, slot):
        return column_copy(wq_hbm, 0, width, core * q_cols + t * TILE, slot)

    def kv_copy(which, slot):
        return column_copy(wkv_hbm, 0, width, (2 * which + core) * TILE, slot)

    def o_copy(t, slot):
        return column_copy(wo_hbm, core * q_cols, q_cols, t * TILE, slot)

    def gate_copy(t, slot):
        return column_copy(wg_hbm, 0, width, t * TILE, slot)

    def up_copy(t, slot):
        return column_copy(wu_hbm, 0, width, t * TILE, slot)

    def down_copy(t, slot):
        return column_copy(wd_hbm, 0, depth, t * TILE, slot)

    def start_ff(i):
        slot = lax.rem(i, SLOTS)
        r = lax.rem(i - ff_first, per_pass)
        live = i < n_tiles

        @pl.when(live & (r < 2 * n_ff) & (lax.rem(r, 2) == 0))
        def _():
            gate_copy(r // 2, slot).start()

        @pl.when(live & (r < 2 * n_ff) & (lax.rem(r, 2) == 1))
        def _():
            up_copy(r // 2, slot).start()

        @pl.when(live & (r >= 2 * n_ff))
        def _():
            down_copy(r - 2 * n_ff, slot).start()

    def each_kv(i, act):
        buf = lax.rem(i, KV_BUFS)
        at = (pl.ds(base + lax.rem(i, n_groups) * SEQS, SEQS), pl.ds(core * kv_heads, kv_heads))

        @pl.when(i < n_groups)
        def _():
            act(pltpu.make_async_copy(k_hbm.at[at], kv_buf.at[buf], kv_sem.at[buf]))

        @pl.when((i >= n_groups) & (i < 2 * n_groups))
        def _():
            act(pltpu.make_async_copy(v_hbm.at[at], kv_buf.at[buf], kv_sem.at[buf]))

    def start_kv(i):
        each_kv(i, lambda copy: copy.start())

    def wait_kv(i):
        each_kv(i, lambda copy: copy.wait())

    x_copy = pltpu.make_async_copy(x_hbm.at[pl.ds(base, pair)], x_s, x_sem)
    x_copy.start()
    for t in range(AHEAD):
        q_copy(t, t).start()

    def signal(target):
        pl.semaphore_signal(pltpu.get_barrier_semaphore(), inc=1, device_id=target, device_id_type=MESH)

    signal({'side': partner})

    @pl.when(is_end)
    def _():
        signal({'dev': mid_dev})
        pl.semaphore_wait(pltpu.get_barrier_semaphore(), 2)

    @pl.when(is_mid)
    def _():
        signal({'dev': end_dev})
        signal({'dev': far_dev})
        pl.semaphore_wait(pltpu.get_barrier_semaphore(), 3)


    def lookup(i, carry):
        n = len_ref[base + i]
        cos_s[pl.ds(i, 1), :] = cos_tab[n]
        sin_s[pl.ds(i, 1), :] = sin_tab[n]
        return carry

    lax.fori_loop(0, pair, lookup, 0)
    x_copy.wait()
    x_f = x_s[...].astype(jnp.float32)
    inv = lax.rsqrt(jnp.mean(x_f * x_f, axis=-1, keepdims=True) + EPS)
    a_s[...] = (x_f * inv * gain_ref[...]).astype(jnp.bfloat16)

    def rotated(tile, i):
        vec = tile[:, i * head:(i + 1) * head]
        return vec * cos_s[...] + pltpu.roll(vec, head // 2, 1) * sin_s[...]

    def q_step(t, carry):
        q_copy(t, t).wait()
        ahead = t + AHEAD

        @pl.when(ahead < n_q)
        def _():
            q_copy(ahead, ahead).start()

        for which in range(2):
            @pl.when(ahead == n_q + which)
            def _():
                kv_copy(which, n_q + which).start()

        for i in range(KV_BUFS):
            @pl.when(t == n_q - 1)
            def _():
                start_kv(i)

        tile = jnp.dot(a_s[...], ring[t], preferred_element_type=jnp.float32)
        for i in range(TILE // head):
            q_s[:, pl.ds(pl.multiple_of(t * TILE + i * head, head), head)] = rotated(tile, i)
        return carry

    lax.fori_loop(0, n_q, q_step, 0)
    kv_copy(0, n_q).wait()
    tile = jnp.dot(a_s[...], ring[n_q], preferred_element_type=jnp.float32)
    for i in range(TILE // head):
        kv_s[:, i * head:(i + 1) * head] = rotated(tile, i)
    kv_copy(1, n_q + 1).wait()
    kv_s[:, TILE:] = jnp.dot(a_s[...], ring[n_q + 1], preferred_element_type=jnp.float32)

    scale = head ** -0.5
    keys = kv_heads * cache
    row_head = lax.broadcasted_iota(jnp.int32, (heads, keys), 0) // group
    col = lax.broadcasted_iota(jnp.int32, (heads, keys), 1)
    key_pos = jnp.where(col // cache == row_head, col % cache, cache + 1)
    nt = (((1,), (1,)), ((), ()))

    def seq_rows(i):
        return pl.ds(pl.multiple_of(i * heads, heads), heads)

    def group_rows(g):
        return pl.ds(pl.multiple_of(g * SEQS, SEQS), SEQS)

    def spread_heads(g, first_col):
        for h in range(heads):
            at = first_col + (h // group) * head
            tx[pl.ds(h, SEQS, stride=heads), :] = kv_s[group_rows(g), at:at + head]
        return tx[...].astype(jnp.bfloat16).astype(jnp.float32)

    def score_group(g, carry):
        buf = lax.rem(g, KV_BUFS)
        for h in range(heads):
            tq[pl.ds(h, SEQS, stride=heads), :] = q_s[group_rows(g), h * head:(h + 1) * head]
        q = tq[...].astype(jnp.bfloat16)
        tb[...] = q
        s_own = jnp.sum(q.astype(jnp.float32) * spread_heads(g, 0), axis=-1, keepdims=True) * scale
        s_s[g, :, keys:] = jnp.broadcast_to(s_own, (SEQS * heads, head))
        wait_kv(g)

        def one(i, carry):
            k = kv_buf[buf, i].reshape(keys, head)
            s_s[g, seq_rows(i), :keys] = lax.dot_general(tb[seq_rows(i), :], k, nt, preferred_element_type=jnp.float32)
            return carry

        lax.fori_loop(0, SEQS, one, 0, unroll=True)
        start_kv(g + KV_BUFS)
        return carry

    def softmax_group(g, carry):
        o_copy(g, lax.rem(o_first + g, SLOTS)).start()

        def one(i, carry):
            n = len_ref[base + g * SEQS + i]
            s = jnp.where(key_pos < n, s_s[g, seq_rows(i), :keys] * scale, -1e30)
            s_own = s_s[g, seq_rows(i), keys:]
            top = jnp.maximum(jnp.max(s, axis=-1, keepdims=True), s_own)
            e = jnp.exp(s - top[:, :1])
            e_own = jnp.exp(s_own - top)
            p_s[g, seq_rows(i), :] = e.astype(jnp.bfloat16)
            s_s[g, seq_rows(i), :head] = jnp.sum(e, axis=-1, keepdims=True) + e_own
            s_s[g, seq_rows(i), keys:] = e_own.astype(jnp.bfloat16).astype(jnp.float32)
            return carry

        lax.fori_loop(0, SEQS, one, 0, unroll=True)
        return carry

    def mix_group(g, carry):
        buf = lax.rem(n_groups + g, KV_BUFS)
        wait_kv(n_groups + g)

        def one(i, carry):
            v = kv_buf[buf, i].reshape(keys, head)
            tq[seq_rows(i), :] = jnp.dot(p_s[g, seq_rows(i), :], v, preferred_element_type=jnp.float32)
            return carry

        lax.fori_loop(0, SEQS, one, 0, unroll=True)
        start_kv(n_groups + g + KV_BUFS)
        tq[...] = (tq[...] + s_s[g, :, keys:] * spread_heads(g, TILE)) / s_s[g, :, :head]
        for h in range(heads):
            q_s[group_rows(g), h * head:(h + 1) * head] = tq[pl.ds(h, SEQS, stride=heads), :]
        return carry

    lax.fori_loop(0, n_groups, score_group, 0)
    lax.fori_loop(0, n_groups, softmax_group, 0)
    lax.fori_loop(0, n_groups, mix_group, 0)
    ob_s[...] = q_s[...].astype(jnp.bfloat16)

    def give(t):
        return pltpu.make_async_remote_copy(
            src_ref=part.at[1, t], dst_ref=take_s.at[t], send_sem=give_sem.at[t], recv_sem=take_sem.at[t],
            device_id={'side': partner}, device_id_type=MESH)

    def o_step(t, carry):
        slot = lax.rem(o_first + t, SLOTS)
        o_copy(t, slot).wait()
        y = jnp.dot(ob_s[...], ring[slot, :q_cols], preferred_element_type=jnp.float32)
        part[1, t] = jnp.where(core == 0, y[rows:], y[:rows])
        give(t).start()
        part[0, t] = jnp.where(core == 0, y[:rows], y[rows:])
        start_ff(ff_first - o_first + o_first + t)
        return carry

    lax.fori_loop(0, n_col, o_step, 0)
    own_rows = pl.ds(pl.multiple_of(core * rows, rows), rows)

    def x1_step(t, square):
        give(t).wait_recv()
        give(t).wait_send()
        cols = pl.ds(pl.multiple_of(t * TILE, TILE), TILE)
        x1 = (x_s[own_rows, cols].astype(jnp.float32) + (part[0, t] + take_s[t])).astype(jnp.bfloat16)
        x1_s[:, cols] = x1
        x1_f = x1.astype(jnp.float32)
        return square + jnp.sum(x1_f * x1_f, axis=-1, keepdims=True)

    square = lax.fori_loop(0, n_col, x1_step, jnp.zeros((rows, 1), jnp.float32))
    inv = lax.rsqrt(square / width + EPS)
    me = jnp.where(is_end, 0, 1)
    h_all[me] = (x1_s[...].astype(jnp.float32) * inv * ffn_gain_ref[...]).astype(jnp.bfloat16)

    def send_h(src, dst, k, target):
        return pltpu.make_async_remote_copy(
            src_ref=h_all.at[src], dst_ref=h_all.at[dst], send_sem=h_send.at[k], recv_sem=h_recv.at[dst],
            device_id={'dev': target}, device_id_type=MESH)

    def send_part(j, c, slot, target):
        return pltpu.make_async_remote_copy(
            src_ref=part.at[j, c], dst_ref=recv.at[slot, c], send_sem=p_send.at[j, c], recv_sem=p_recv.at[slot, c],
            device_id={'dev': target}, device_id_type=MESH)

    @pl.when(is_end)
    def _():
        send_h(0, 0, 0, mid_dev).start()
        send_h(0, 1, 0, mid_dev).wait_recv()

    @pl.when(is_mid)
    def _():
        send_h(1, 1, 0, end_dev).start()
        send_h(1, 2, 1, far_dev).start()
        send_h(1, 0, 0, end_dev).wait_recv()
        send_h(0, 3, 2, far_dev).start()
        send_h(1, 2, 0, end_dev).wait_recv()
        send_h(2, 2, 3, end_dev).start()

    for half in range(2):
        def ff_step(t, carry):
            i = ff_first + half * per_pass + 2 * t
            slot_g, slot_u = lax.rem(i, SLOTS), lax.rem(i + 1, SLOTS)
            h = h_all[2 * half:2 * half + 2].reshape(2 * rows, width)
            gate_copy(t, slot_g).wait()
            gate = jnp.dot(h, ring[slot_g], preferred_element_type=jnp.float32)
            start_ff(i + SLOTS)
            up_copy(t, slot_u).wait()
            up = jnp.dot(h, ring[slot_u], preferred_element_type=jnp.float32)
            start_ff(i + 1 + SLOTS)
            u_s[:, pl.ds(pl.multiple_of(t * TILE, TILE), TILE)] = (jax.nn.silu(gate) * up).astype(jnp.bfloat16)
            return carry

        def down_step(c, carry):
            i = ff_first + half * per_pass + 2 * n_ff + c
            slot = lax.rem(i, SLOTS)
            down_copy(c, slot).wait()
            y = jnp.dot(u_s[...], ring[slot, :depth], preferred_element_type=jnp.float32)
            start_ff(i + SLOTS)
            part[2 * half, c] = y[:rows]
            part[2 * half + 1, c] = y[rows:]

            @pl.when(is_end)
            def _():
                send_part(2 * half + 1, c, 2 * half, mid_dev).start()

            if half == 0:
                @pl.when(is_mid & (c == n_col - 3))
                def _():
                    send_h(1, 3, 0, end_dev).wait_recv()
                    send_h(3, 3, 4, end_dev).start()

            return carry

        if half == 1:
            @pl.when(is_end)
            def _():
                send_h(0, 2, 0, mid_dev).wait_recv()
                send_h(0, 3, 0, mid_dev).wait_recv()

        lax.fori_loop(0, n_ff, ff_step, 0)
        lax.fori_loop(0, n_col, down_step, 0)

    def finish(c, y):
        cols = pl.ds(pl.multiple_of(c * TILE, TILE), TILE)
        y = y.astype(jnp.bfloat16).astype(jnp.float32)
        out_ref[:, cols] = (x1_s[:, cols].astype(jnp.float32) + y).astype(jnp.bfloat16)

    @pl.when(is_end)
    def _():
        def second(c, carry):
            send_part(2, c, 1, mid_dev).start()
            return carry

        def home(c, carry):
            send_part(0, c, 0, mid_dev).wait_recv()
            finish(c, part[0, c] + recv[0, c])
            return carry

        def drain(c, carry):
            for j in (1, 3, 2):
                send_part(j, c, 0, mid_dev).wait_send()
            return carry

        lax.fori_loop(0, n_col, second, 0)
        lax.fori_loop(0, n_col, home, 0)
        lax.fori_loop(0, n_col, drain, 0)
        send_h(0, 0, 0, mid_dev).wait_send()

    @pl.when(is_mid)
    def _():
        def back(c):
            send_part(0, c, 4, far_dev).wait_recv()
            part[0, c] += recv[4, c]
            send_part(0, c, 0, end_dev).start()

        def across(c, carry):
            send_part(3, c, 2, end_dev).wait_recv()
            part[3, c] += recv[2, c]
            send_part(3, c, 4, far_dev).start()

            @pl.when(c > 0)
            def _():
                back(c - 1)

            return carry

        def home(c):
            send_part(1, c, 0, end_dev).wait_recv()
            send_part(1, c, 3, far_dev).wait_recv()
            finish(c, part[1, c] + recv[0, c] + recv[3, c])

        def near(c, carry):
            send_part(2, c, 1, end_dev).wait_recv()
            part[2, c] += recv[1, c]
            send_part(2, c, 3, far_dev).start()

            @pl.when(c > 0)
            def _():
                home(c - 1)

            return carry

        def drain(c, carry):
            for j in (3, 0, 2):
                send_part(j, c, 0, far_dev).wait_send()
            return carry

        lax.fori_loop(0, n_col, across, 0)
        back(n_col - 1)
        lax.fori_loop(0, n_col, near, 0)
        home(n_col - 1)
        lax.fori_loop(0, n_col, drain, 0)
        for k in range(5):
            send_h(0, 0, k, end_dev).wait_send()


def layer_step(hidden, lengths, k_cache, v_cache, w_q, w_kv, w_o, gain_attn, gain_ffn, w_gate, w_up, w_down, n_side):
    rows, width = hidden.shape[0] // n_side, hidden.shape[1]
    _, kv_heads, cache, head = k_cache.shape
    q_cols = w_q.shape[1] // 2
    heads = q_cols // head
    depth = w_down.shape[0]
    n_col = width // TILE
    assert kv_heads * head == 2 * TILE, "tile"
    cos_tab, sin_tab = rope_tables(cache, head)
    vmem = pl.BlockSpec(memory_space=pltpu.VMEM)
    hbm = pl.BlockSpec(memory_space=pl.ANY)
    f32, bf16 = jnp.float32, jnp.bfloat16
    dma = pltpu.SemaphoreType.DMA
    kv_block = (KV_BUFS, SEQS, kv_heads // 2, cache, head)
    return pl.pallas_call(
        functools.partial(layer_kernel, rows),
        out_shape=jax.ShapeDtypeStruct((rows, width), bf16),
        in_specs=[pl.BlockSpec(memory_space=pltpu.SMEM)] + [vmem] * 4 + [hbm] * 9,
        out_specs=vmem,
        scratch_shapes=[
            pltpu.VMEM((SLOTS, width, TILE), bf16),
            pltpu.VMEM(kv_block, bf16),
            pltpu.VMEM((2 * rows, width), bf16),
            pltpu.VMEM((2 * rows, width), bf16),
            pltpu.VMEM((2 * rows, head), f32),
            pltpu.VMEM((2 * rows, head), f32),
            pltpu.VMEM((2 * rows, q_cols), f32),
            pltpu.VMEM((2 * rows, 2 * TILE), f32),
            pltpu.VMEM((2 * rows, q_cols), bf16),
            pltpu.VMEM((2 * rows // SEQS, SEQS * heads, kv_heads // 2 * cache + head), f32),
            pltpu.VMEM((2 * rows // SEQS, SEQS * heads, kv_heads // 2 * cache), bf16),
            pltpu.VMEM((SEQS * heads, head), f32),
            pltpu.VMEM((SEQS * heads, head), f32),
            pltpu.VMEM((SEQS * heads, head), bf16),
            pltpu.VMEM((n_col, rows, TILE), f32),
            pltpu.VMEM((rows, width), bf16),
            pltpu.VMEM((4, rows, width), bf16),
            pltpu.VMEM((2 * rows, depth), bf16),
            pltpu.VMEM((4, n_col, rows, TILE), f32),
            pltpu.VMEM((5, n_col, rows, TILE), f32),
            dma(()),
            dma((SLOTS,)),
            dma((KV_BUFS,)),
            dma((n_col,)),
            dma((n_col,)),
            dma((5,)),
            dma((4,)),
            dma((4, n_col)),
            dma((5, n_col)),
        ],
        compiler_params=pltpu.CompilerParams(vmem_limit_bytes=VMEM_LIMIT, collective_id=0, has_side_effects=True),
        name="layer",
    )(lengths, jnp.asarray(cos_tab), jnp.asarray(sin_tab), gain_attn[None], gain_ffn[None], hidden, k_cache, v_cache,
      w_q, w_kv, w_o, w_gate, w_up, w_down)


def solution(mesh):
    n_side = mesh.shape['side']
    assert n_side == 4 and mesh.shape['dev'] == 4, "mesh"
    batch_axes = ('inst', 'dev')
    in_specs = (
        P(batch_axes, None),
        P(batch_axes),
        P(None, batch_axes, None, None, None),
        P(None, batch_axes, None, None, None),
        P(), P(), P(), P(), P(),
        P(None, None, 'dev'),
        P(None, None, 'dev'),
        P(None, 'dev', None),
    )
    out_specs = P(('inst', 'dev', 'side'), None)

    def device_fn(hidden, cache_len, k_cache, v_cache, w_q, w_kv, w_o, attn_gain, ffn_gain, w_gate, w_up, w_down):
        assert w_q.shape[0] == 1, "layers"
        return layer_step(hidden, cache_len, k_cache[0], v_cache[0], w_q[0], w_kv[0], w_o[0], attn_gain[0], ffn_gain[0],
                          w_gate[0], w_up[0], w_down[0], n_side)

    return jax.shard_map(device_fn, mesh=mesh, in_specs=in_specs, out_specs=out_specs, check_vma=False)
```

```python
import functools

import jax
import jax.numpy as jnp
import numpy as np
from jax import lax
from jax.experimental import pallas as pl
from jax.experimental.pallas import tpu as pltpu
from jax.sharding import PartitionSpec as P

EPS = 1e-5
ROPE_BASE = 10000.0
TILE = 512
SLOTS = 8
SEQS = 16
KV_BUFS = 4
AHEAD = 3
VMEM_LIMIT = 66_000_000
MESH = pl.DeviceIdType.MESH


def rope_tables(cache, head):
    half = head // 2
    freqs = np.power(np.float32(ROPE_BASE), -np.arange(half, dtype=np.float32) / np.float32(half))
    angle = np.arange(cache + 1, dtype=np.float32)[:, None] * freqs.astype(np.float32)
    cos_part, sin_part = np.cos(angle.astype(np.float64)), np.sin(angle.astype(np.float64))
    cos_full = np.concatenate([cos_part, cos_part], axis=-1).astype(np.float32)
    sin_full = np.concatenate([-sin_part, sin_part], axis=-1).astype(np.float32)
    return cos_full[:, None], sin_full[:, None]


def layer_kernel(rows, len_ref, cos_tab, sin_tab, gain_ref, ffn_gain_ref, x_hbm, k_hbm, v_hbm, wq_hbm, wkv_hbm, wo_hbm,
                 wg_hbm, wu_hbm, wd_hbm, out_ref, ring, kv_buf, x_s, a_s, cos_s, sin_s, q_s, kv_s, ob_s, s_s, p_s,
                 tq, tx, tb, take_s, x1_s, h_all, u_s, part, recv, x_sem, w_sem, kv_sem, give_sem, take_sem,
                 h_send, h_recv, p_send, p_recv):
    width = x_hbm.shape[1]
    _, kv_heads, cache, head = k_hbm.shape
    kv_heads //= 2
    q_cols = wq_hbm.shape[1] // 2
    heads = q_cols // head
    group = heads // kv_heads
    pair = 2 * rows
    n_groups = pair // SEQS
    assert n_groups == width // TILE and q_cols // TILE == AHEAD + 1, "groups"
    depth = wd_hbm.shape[0]
    n_q = q_cols // TILE
    n_col = width // TILE
    n_ff = depth // TILE
    o_first = n_q + 2
    ff_first = o_first + n_col
    per_pass = 2 * n_ff + n_col
    n_tiles = ff_first + 2 * per_pass

    side = lax.axis_index('side')
    core = lax.rem(side, 2)
    partner = side + 1 - 2 * core
    base = (side // 2) * pair
    dev = lax.axis_index('dev')
    flip = dev >= 2
    is_end = (dev == 0) | (dev == 3)
    is_mid = (dev == 1) | (dev == 2)
    end_dev = jnp.where(flip, 3, 0)
    mid_dev = jnp.where(flip, 2, 1)
    far_dev = jnp.where(flip, 1, 2)

    def column_copy(hbm, first_row, n_rows, first_col, slot):
        cols = pl.ds(pl.multiple_of(first_col, TILE), TILE)
        return pltpu.make_async_copy(hbm.at[pl.ds(first_row, n_rows), cols], ring.at[slot, pl.ds(0, n_rows)],
                                     w_sem.at[slot])

    def q_copy(t, slot):
        return column_copy(wq_hbm, 0, width, core * q_cols + t * TILE, slot)

    def kv_copy(which, slot):
        return column_copy(wkv_hbm, 0, width, (2 * which + core) * TILE, slot)

    def o_copy(t, slot):
        return column_copy(wo_hbm, core * q_cols, q_cols, t * TILE, slot)

    def gate_copy(t, slot):
        return column_copy(wg_hbm, 0, width, t * TILE, slot)

    def up_copy(t, slot):
        return column_copy(wu_hbm, 0, width, t * TILE, slot)

    def down_copy(t, slot):
        return column_copy(wd_hbm, 0, depth, t * TILE, slot)

    def start_ff(i):
        slot = lax.rem(i, SLOTS)
        r = lax.rem(i - ff_first, per_pass)
        live = i < n_tiles

        @pl.when(live & (r < 2 * n_ff) & (lax.rem(r, 2) == 0))
        def _():
            gate_copy(r // 2, slot).start()

        @pl.when(live & (r < 2 * n_ff) & (lax.rem(r, 2) == 1))
        def _():
            up_copy(r // 2, slot).start()

        @pl.when(live & (r >= 2 * n_ff))
        def _():
            down_copy(r - 2 * n_ff, slot).start()

    def each_kv(i, act):
        buf = lax.rem(i, KV_BUFS)
        at = (pl.ds(base + lax.rem(i, n_groups) * SEQS, SEQS), pl.ds(core * kv_heads, kv_heads))

        @pl.when(i < n_groups)
        def _():
            act(pltpu.make_async_copy(k_hbm.at[at], kv_buf.at[buf], kv_sem.at[buf]))

        @pl.when((i >= n_groups) & (i < 2 * n_groups))
        def _():
            act(pltpu.make_async_copy(v_hbm.at[at], kv_buf.at[buf], kv_sem.at[buf]))

    def start_kv(i):
        each_kv(i, lambda copy: copy.start())

    def wait_kv(i):
        each_kv(i, lambda copy: copy.wait())

    x_copy = pltpu.make_async_copy(x_hbm.at[pl.ds(base, pair)], x_s, x_sem)
    x_copy.start()
    for t in range(AHEAD):
        q_copy(t, t).start()

    def signal(target):
        pl.semaphore_signal(pltpu.get_barrier_semaphore(), inc=1, device_id=target, device_id_type=MESH)

    signal({'side': partner})

    @pl.when(is_end)
    def _():
        signal({'dev': mid_dev})
        pl.semaphore_wait(pltpu.get_barrier_semaphore(), 2)

    @pl.when(is_mid)
    def _():
        signal({'dev': end_dev})
        signal({'dev': far_dev})
        pl.semaphore_wait(pltpu.get_barrier_semaphore(), 3)


    def lookup(i, carry):
        n = len_ref[base + i]
        cos_s[pl.ds(i, 1), :] = cos_tab[n]
        sin_s[pl.ds(i, 1), :] = sin_tab[n]
        return carry

    lax.fori_loop(0, pair, lookup, 0, unroll=8)
    x_copy.wait()
    x_f = x_s[...].astype(jnp.float32)
    inv = lax.rsqrt(jnp.mean(x_f * x_f, axis=-1, keepdims=True) + EPS)
    a_s[...] = (x_f * inv * gain_ref[...]).astype(jnp.bfloat16)

    def rotated(tile, i):
        vec = tile[:, i * head:(i + 1) * head]
        return vec * cos_s[...] + pltpu.roll(vec, head // 2, 1) * sin_s[...]

    def q_step(t, carry):
        q_copy(t, t).wait()
        ahead = t + AHEAD

        @pl.when(ahead < n_q)
        def _():
            q_copy(ahead, ahead).start()

        for which in range(2):
            @pl.when(ahead == n_q + which)
            def _():
                kv_copy(which, n_q + which).start()

        for i in range(KV_BUFS):
            @pl.when(t == n_q - 1)
            def _():
                start_kv(i)

        tile = jnp.dot(a_s[...], ring[t], preferred_element_type=jnp.float32)
        for i in range(TILE // head):
            q_s[:, pl.ds(pl.multiple_of(t * TILE + i * head, head), head)] = rotated(tile, i)
        return carry

    lax.fori_loop(0, n_q, q_step, 0)
    kv_copy(0, n_q).wait()
    tile = jnp.dot(a_s[...], ring[n_q], preferred_element_type=jnp.float32)
    for i in range(TILE // head):
        kv_s[:, i * head:(i + 1) * head] = rotated(tile, i)
    kv_copy(1, n_q + 1).wait()
    kv_s[:, TILE:] = jnp.dot(a_s[...], ring[n_q + 1], preferred_element_type=jnp.float32)

    scale = head ** -0.5
    keys = kv_heads * cache
    row_head = lax.broadcasted_iota(jnp.int32, (heads, keys), 0) // group
    col = lax.broadcasted_iota(jnp.int32, (heads, keys), 1)
    key_pos = jnp.where(col // cache == row_head, col % cache, cache + 1)
    nt = (((1,), (1,)), ((), ()))

    def seq_rows(i):
        return pl.ds(pl.multiple_of(i * heads, heads), heads)

    def group_rows(g):
        return pl.ds(pl.multiple_of(g * SEQS, SEQS), SEQS)

    def spread_heads(g, first_col):
        for h in range(heads):
            at = first_col + (h // group) * head
            tx[pl.ds(h, SEQS, stride=heads), :] = kv_s[group_rows(g), at:at + head]
        return tx[...].astype(jnp.bfloat16).astype(jnp.float32)

    def score_group(g, carry):
        buf = lax.rem(g, KV_BUFS)
        for h in range(heads):
            tq[pl.ds(h, SEQS, stride=heads), :] = q_s[group_rows(g), h * head:(h + 1) * head]
        q = tq[...].astype(jnp.bfloat16)
        tb[...] = q
        s_own = jnp.sum(q.astype(jnp.float32) * spread_heads(g, 0), axis=-1, keepdims=True) * scale
        s_s[g, :, keys:] = jnp.broadcast_to(s_own, (SEQS * heads, head))
        wait_kv(g)

        def one(i, carry):
            k = kv_buf[buf, i].reshape(keys, head)
            s_s[g, seq_rows(i), :keys] = lax.dot_general(tb[seq_rows(i), :], k, nt, preferred_element_type=jnp.float32)
            return carry

        lax.fori_loop(0, SEQS, one, 0, unroll=True)
        start_kv(g + KV_BUFS)
        return carry

    def softmax_group(g, carry):
        o_copy(g, lax.rem(o_first + g, SLOTS)).start()

        def one(i, carry):
            n = len_ref[base + g * SEQS + i]
            s = jnp.where(key_pos < n, s_s[g, seq_rows(i), :keys] * scale, -1e30)
            s_own = s_s[g, seq_rows(i), keys:]
            top = jnp.maximum(jnp.max(s, axis=-1, keepdims=True), s_own)
            e = jnp.exp(s - top[:, :1])
            e_own = jnp.exp(s_own - top)
            p_s[g, seq_rows(i), :] = e.astype(jnp.bfloat16)
            s_s[g, seq_rows(i), :head] = jnp.sum(e, axis=-1, keepdims=True) + e_own
            s_s[g, seq_rows(i), keys:] = e_own.astype(jnp.bfloat16).astype(jnp.float32)
            return carry

        lax.fori_loop(0, SEQS, one, 0, unroll=True)
        return carry

    def mix_group(g, carry):
        buf = lax.rem(n_groups + g, KV_BUFS)
        wait_kv(n_groups + g)

        def one(i, carry):
            v = kv_buf[buf, i].reshape(keys, head)
            tq[seq_rows(i), :] = jnp.dot(p_s[g, seq_rows(i), :], v, preferred_element_type=jnp.float32)
            return carry

        lax.fori_loop(0, SEQS, one, 0, unroll=True)
        start_kv(n_groups + g + KV_BUFS)
        tq[...] = (tq[...] + s_s[g, :, keys:] * spread_heads(g, TILE)) / s_s[g, :, :head]
        for h in range(heads):
            q_s[group_rows(g), h * head:(h + 1) * head] = tq[pl.ds(h, SEQS, stride=heads), :]
        return carry

    lax.fori_loop(0, n_groups, score_group, 0)
    lax.fori_loop(0, n_groups, softmax_group, 0)
    lax.fori_loop(0, n_groups, mix_group, 0)
    ob_s[...] = q_s[...].astype(jnp.bfloat16)

    def give(t):
        return pltpu.make_async_remote_copy(
            src_ref=part.at[1, t], dst_ref=take_s.at[t], send_sem=give_sem.at[t], recv_sem=take_sem.at[t],
            device_id={'side': partner}, device_id_type=MESH)

    def o_step(t, carry):
        slot = lax.rem(o_first + t, SLOTS)
        o_copy(t, slot).wait()
        y = jnp.dot(ob_s[...], ring[slot, :q_cols], preferred_element_type=jnp.float32)
        part[1, t] = jnp.where(core == 0, y[rows:], y[:rows])
        give(t).start()
        part[0, t] = jnp.where(core == 0, y[:rows], y[rows:])
        return carry

    lax.fori_loop(0, n_col, o_step, 0)
    own_rows = pl.ds(pl.multiple_of(core * rows, rows), rows)

    def x1_step(t, square):
        give(t).wait_recv()
        give(t).wait_send()
        cols = pl.ds(pl.multiple_of(t * TILE, TILE), TILE)
        x1 = (x_s[own_rows, cols].astype(jnp.float32) + (part[0, t] + take_s[t])).astype(jnp.bfloat16)
        x1_s[:, cols] = x1
        x1_f = x1.astype(jnp.float32)
        start_ff(ff_first + t)
        return square + jnp.sum(x1_f * x1_f, axis=-1, keepdims=True)

    square = lax.fori_loop(0, n_col, x1_step, jnp.zeros((rows, 1), jnp.float32))
    inv = lax.rsqrt(square / width + EPS)
    me = jnp.where(is_end, 0, 1)
    h_all[me] = (x1_s[...].astype(jnp.float32) * inv * ffn_gain_ref[...]).astype(jnp.bfloat16)

    def send_h(src, dst, k, target):
        return pltpu.make_async_remote_copy(
            src_ref=h_all.at[src], dst_ref=h_all.at[dst], send_sem=h_send.at[k], recv_sem=h_recv.at[dst],
            device_id={'dev': target}, device_id_type=MESH)

    def send_part(j, c, slot, target):
        return pltpu.make_async_remote_copy(
            src_ref=part.at[j, c], dst_ref=recv.at[slot, c], send_sem=p_send.at[j, c], recv_sem=p_recv.at[slot, c],
            device_id={'dev': target}, device_id_type=MESH)

    @pl.when(is_end)
    def _():
        send_h(0, 0, 0, mid_dev).start()
        send_h(0, 1, 0, mid_dev).wait_recv()

    @pl.when(is_mid)
    def _():
        send_h(1, 1, 0, end_dev).start()
        send_h(1, 2, 1, far_dev).start()
        send_h(1, 0, 0, end_dev).wait_recv()
        send_h(0, 3, 2, far_dev).start()
        send_h(1, 2, 0, end_dev).wait_recv()
        send_h(2, 2, 3, end_dev).start()

    for half in range(2):
        def ff_step(t, carry):
            i = ff_first + half * per_pass + 2 * t
            slot_g, slot_u = lax.rem(i, SLOTS), lax.rem(i + 1, SLOTS)
            h = h_all[2 * half:2 * half + 2].reshape(2 * rows, width)
            gate_copy(t, slot_g).wait()
            gate = jnp.dot(h, ring[slot_g], preferred_element_type=jnp.float32)
            start_ff(i + SLOTS)
            up_copy(t, slot_u).wait()
            up = jnp.dot(h, ring[slot_u], preferred_element_type=jnp.float32)
            start_ff(i + 1 + SLOTS)
            u_s[:, pl.ds(pl.multiple_of(t * TILE, TILE), TILE)] = (jax.nn.silu(gate) * up).astype(jnp.bfloat16)
            return carry

        def down_step(c, carry):
            i = ff_first + half * per_pass + 2 * n_ff + c
            slot = lax.rem(i, SLOTS)
            down_copy(c, slot).wait()
            y = jnp.dot(u_s[...], ring[slot, :depth], preferred_element_type=jnp.float32)
            start_ff(i + SLOTS)
            part[2 * half, c] = y[:rows]
            part[2 * half + 1, c] = y[rows:]

            @pl.when(is_end)
            def _():
                send_part(2 * half + 1, c, 2 * half, mid_dev).start()

            if half == 0:
                @pl.when(is_mid & (c == 1))
                def _():
                    send_h(1, 3, 0, end_dev).wait_recv()
                    send_h(3, 3, 4, end_dev).start()

            return carry

        if half == 1:
            @pl.when(is_end)
            def _():
                send_h(0, 2, 0, mid_dev).wait_recv()
                send_h(0, 3, 0, mid_dev).wait_recv()

        lax.fori_loop(0, n_ff, ff_step, 0)
        lax.fori_loop(0, n_col, down_step, 0)

    def finish(c, y):
        cols = pl.ds(pl.multiple_of(c * TILE, TILE), TILE)
        y = y.astype(jnp.bfloat16).astype(jnp.float32)
        out_ref[:, cols] = (x1_s[:, cols].astype(jnp.float32) + y).astype(jnp.bfloat16)

    @pl.when(is_end)
    def _():
        def second(c, carry):
            send_part(2, c, 1, mid_dev).start()
            return carry

        def home(c, carry):
            send_part(0, c, 0, mid_dev).wait_recv()
            finish(c, part[0, c] + recv[0, c])
            return carry

        def drain(c, carry):
            for j in (1, 3, 2):
                send_part(j, c, 0, mid_dev).wait_send()
            return carry

        lax.fori_loop(0, n_col, second, 0)
        lax.fori_loop(0, n_col, home, 0)
        lax.fori_loop(0, n_col, drain, 0)
        send_h(0, 0, 0, mid_dev).wait_send()

    @pl.when(is_mid)
    def _():
        def back(c):
            send_part(0, c, 4, far_dev).wait_recv()
            part[0, c] += recv[4, c]
            send_part(0, c, 0, end_dev).start()

        def across(c, carry):
            send_part(3, c, 2, end_dev).wait_recv()
            part[3, c] += recv[2, c]
            send_part(3, c, 4, far_dev).start()

            @pl.when(c > 0)
            def _():
                back(c - 1)

            return carry

        def home(c):
            send_part(1, c, 0, end_dev).wait_recv()
            send_part(1, c, 3, far_dev).wait_recv()
            finish(c, part[1, c] + recv[0, c] + recv[3, c])

        def near(c, carry):
            send_part(2, c, 1, end_dev).wait_recv()
            part[2, c] += recv[1, c]
            send_part(2, c, 3, far_dev).start()

            @pl.when(c > 0)
            def _():
                home(c - 1)

            return carry

        def drain(c, carry):
            for j in (3, 0, 2):
                send_part(j, c, 0, far_dev).wait_send()
            return carry

        lax.fori_loop(0, n_col, across, 0)
        back(n_col - 1)
        lax.fori_loop(0, n_col, near, 0)
        home(n_col - 1)
        lax.fori_loop(0, n_col, drain, 0)
        for k in range(5):
            send_h(0, 0, k, end_dev).wait_send()


def layer_step(hidden, lengths, k_cache, v_cache, w_q, w_kv, w_o, gain_attn, gain_ffn, w_gate, w_up, w_down, n_side):
    rows, width = hidden.shape[0] // n_side, hidden.shape[1]
    _, kv_heads, cache, head = k_cache.shape
    q_cols = w_q.shape[1] // 2
    heads = q_cols // head
    depth = w_down.shape[0]
    n_col = width // TILE
    assert kv_heads * head == 2 * TILE, "tile"
    cos_tab, sin_tab = rope_tables(cache, head)
    vmem = pl.BlockSpec(memory_space=pltpu.VMEM)
    hbm = pl.BlockSpec(memory_space=pl.ANY)
    f32, bf16 = jnp.float32, jnp.bfloat16
    dma = pltpu.SemaphoreType.DMA
    kv_block = (KV_BUFS, SEQS, kv_heads // 2, cache, head)
    return pl.pallas_call(
        functools.partial(layer_kernel, rows),
        out_shape=jax.ShapeDtypeStruct((rows, width), bf16),
        in_specs=[pl.BlockSpec(memory_space=pltpu.SMEM)] + [vmem] * 4 + [hbm] * 9,
        out_specs=vmem,
        scratch_shapes=[
            pltpu.VMEM((SLOTS, width, TILE), bf16),
            pltpu.VMEM(kv_block, bf16),
            pltpu.VMEM((2 * rows, width), bf16),
            pltpu.VMEM((2 * rows, width), bf16),
            pltpu.VMEM((2 * rows, head), f32),
            pltpu.VMEM((2 * rows, head), f32),
            pltpu.VMEM((2 * rows, q_cols), f32),
            pltpu.VMEM((2 * rows, 2 * TILE), f32),
            pltpu.VMEM((2 * rows, q_cols), bf16),
            pltpu.VMEM((2 * rows // SEQS, SEQS * heads, kv_heads // 2 * cache + head), f32),
            pltpu.VMEM((2 * rows // SEQS, SEQS * heads, kv_heads // 2 * cache), bf16),
            pltpu.VMEM((SEQS * heads, head), f32),
            pltpu.VMEM((SEQS * heads, head), f32),
            pltpu.VMEM((SEQS * heads, head), bf16),
            pltpu.VMEM((n_col, rows, TILE), f32),
            pltpu.VMEM((rows, width), bf16),
            pltpu.VMEM((4, rows, width), bf16),
            pltpu.VMEM((2 * rows, depth), bf16),
            pltpu.VMEM((4, n_col, rows, TILE), f32),
            pltpu.VMEM((5, n_col, rows, TILE), f32),
            dma(()),
            dma((SLOTS,)),
            dma((KV_BUFS,)),
            dma((n_col,)),
            dma((n_col,)),
            dma((5,)),
            dma((4,)),
            dma((4, n_col)),
            dma((5, n_col)),
        ],
        compiler_params=pltpu.CompilerParams(vmem_limit_bytes=VMEM_LIMIT, collective_id=0, has_side_effects=True),
        name="layer",
    )(lengths, jnp.asarray(cos_tab), jnp.asarray(sin_tab), gain_attn[None], gain_ffn[None], hidden, k_cache, v_cache,
      w_q, w_kv, w_o, w_gate, w_up, w_down)


def solution(mesh):
    n_side = mesh.shape['side']
    assert n_side == 4 and mesh.shape['dev'] == 4, "mesh"
    batch_axes = ('inst', 'dev')
    in_specs = (
        P(batch_axes, None),
        P(batch_axes),
        P(None, batch_axes, None, None, None),
        P(None, batch_axes, None, None, None),
        P(), P(), P(), P(), P(),
        P(None, None, 'dev'),
        P(None, None, 'dev'),
        P(None, 'dev', None),
    )
    out_specs = P(('inst', 'dev', 'side'), None)

    def device_fn(hidden, cache_len, k_cache, v_cache, w_q, w_kv, w_o, attn_gain, ffn_gain, w_gate, w_up, w_down):
        assert w_q.shape[0] == 1, "layers"
        return layer_step(hidden, cache_len, k_cache[0], v_cache[0], w_q[0], w_kv[0], w_o[0], attn_gain[0], ffn_gain[0],
                          w_gate[0], w_up[0], w_down[0], n_side)

    return jax.shard_map(device_fn, mesh=mesh, in_specs=in_specs, out_specs=out_specs, check_vma=False)
```
